32 devices in a mesh: col: 4 (over z), row: 8 (over y, x, core).
Axes of the slice: x: 2, y: 2, z: 4, core: 2. Of those that a mesh axis runs over, the one named last changes fastest.
Arguments:
- w_gate: float32 [768, 2048], P('row', 'col')
- w_up: float32 [768, 2048], P('row', 'col')
- w_down: float32 [2048, 768], P('row', 'col')
- x_norm: bfloat16 [32768, 768], P(None, 'row')
- x_act: bfloat16 [32768, 2048], P(None, 'row')
- dy_gate: bfloat16 [32768, 2048], P(None, 'col')
- dy_up: bfloat16 [32768, 2048], P(None, 'col')
- dy_down: bfloat16 [32768, 768], P(None, 'col')
- r_gate: float32 [768], P('row')
- c_gate: float32 [2048], P('col')
- r_up: float32 [768], P('row')
- c_up: float32 [2048], P('col')
- r_down: float32 [2048], P('row')
- c_down: float32 [768], P('col')
- hyper_params: float32 [3], replicated
Outputs:
- output 1: float32 [768, 2048], P('row', 'col')
- output 2: float32 [768, 2048], P('row', 'col')
- output 3: float32 [2048, 768], P('row', 'col')
- output 4: float32 [768], P('row')
- output 5: float32 [2048], P('col')
- output 6: float32 [768], P('row')
- output 7: float32 [2048], P('col')
- output 8: float32 [2048], P('row')
- output 9: float32 [768], P('col')
- output 10: bfloat16 [32768, 768], P(None, 'row')
- output 11: bfloat16 [32768, 2048], P(None, 'row')
All inputs are finite; a program needn't handle non-finite values.
Results may differ from the reference program's by a relative error of at most 0.001.
Values are sent between devices in bfloat16 or wider.
A program may use at most 1 GiB of HBM per device.

```python
import jax
import jax.numpy as jnp
from jax import lax

D_MODEL = 768
D_FF = 2048
TOKENS = 32768
EPS_ONE = 1e-30
EPS_TWO = 1e-3
TWO_PI = 6.283185307179586


def smooth_field(key, length, log_scale):
    key_amp, key_phase = jax.random.split(key)
    ampl_k = jax.random.normal(key_amp, (3,), jnp.float32)
    phase_k = jax.random.uniform(key_phase, (3,), jnp.float32, minval=0.0, maxval=TWO_PI)
    position = jnp.arange(length, dtype=jnp.float32) / length
    freq_k = jnp.arange(1, 4, dtype=jnp.float32)
    waves = jnp.cos(TWO_PI * position[:, None] * freq_k[None, :] + phase_k[None, :])
    return jnp.exp(log_scale * jnp.sum(waves * ampl_k[None, :], axis=1) / 1.7)


def draw_weight(key, rows, cols):
    key_z, key_r, key_c = jax.random.split(key, 3)
    noise = jax.random.normal(key_z, (rows, cols), jnp.float32)
    row_prof = smooth_field(key_r, rows, 0.5)
    col_prof = smooth_field(key_c, cols, 0.5)
    return noise * (rows ** -0.5) * row_prof[:, None] * col_prof[None, :]


def draw_tokens(key, cols, scale):
    key_z, key_a, key_b = jax.random.split(key, 3)
    noise = jax.random.normal(key_z, (TOKENS, cols), jnp.float32)
    first_half = (jnp.arange(TOKENS) < TOKENS // 2)[:, None]
    profile = jnp.where(first_half, smooth_field(key_a, cols, 0.8)[None, :], smooth_field(key_b, cols, 0.8)[None, :])
    return (noise * profile * scale).astype(jnp.bfloat16)


def draw_stat(key, length):
    return jax.random.uniform(key, (length,), jnp.float32, minval=0.5, maxval=3.0)


def setup_inputs(seed: int = 0) -> dict:
    keys = jax.random.split(jax.random.key(seed), 15)
    tok_scale = TOKENS ** -0.5
    low_end = jnp.array([0.6, 0.6, 0.15], dtype=jnp.float32)
    span_len = jnp.array([0.25, 0.6, 0.15], dtype=jnp.float32)
    unit_draw = jax.random.uniform(keys[14], (3,), jnp.float32)
    return {
        'w_gate': draw_weight(keys[0], D_MODEL, D_FF),
        'w_up': draw_weight(keys[1], D_MODEL, D_FF),
        'w_down': draw_weight(keys[2], D_FF, D_MODEL),
        'x_norm': draw_tokens(keys[3], D_MODEL, tok_scale),
        'x_act': draw_tokens(keys[4], D_FF, tok_scale),
        'dy_gate': draw_tokens(keys[5], D_FF, 1.0),
        'dy_up': draw_tokens(keys[6], D_FF, 1.0),
        'dy_down': draw_tokens(keys[7], D_MODEL, 1.0),
        'r_gate': draw_stat(keys[8], D_MODEL),
        'c_gate': draw_stat(keys[9], D_FF),
        'r_up': draw_stat(keys[10], D_MODEL),
        'c_up': draw_stat(keys[11], D_FF),
        'r_down': draw_stat(keys[12], D_FF),
        'c_down': draw_stat(keys[13], D_MODEL),
        'hyper_params': low_end + span_len * unit_draw,
    }


def factored_step(w_old, grad_w, r_old, c_old, hyper_params):
    beta_two = hyper_params[0]
    grad_sq = grad_w * grad_w + EPS_ONE
    r_new = beta_two * r_old + (1.0 - beta_two) * jnp.mean(grad_sq, axis=1)
    c_new = beta_two * c_old + (1.0 - beta_two) * jnp.mean(grad_sq, axis=0)
    v_est = r_new[:, None] * c_new[None, :] / jnp.mean(r_new)
    update = grad_w * lax.rsqrt(v_est)
    rms_u = jnp.sqrt(jnp.mean(update * update))
    update_hat = update / jnp.maximum(1.0, rms_u / hyper_params[2])
    step_size = hyper_params[1] * jnp.maximum(EPS_TWO, jnp.sqrt(jnp.mean(w_old * w_old)))
    return w_old - step_size * update_hat, r_new, c_new


def weight_grad(activations, grad_out):
    return jnp.dot(activations.T, grad_out, preferred_element_type=jnp.float32)


def input_grad(grad_out, weight):
    return jnp.dot(grad_out, weight.astype(jnp.bfloat16).T, preferred_element_type=jnp.float32)


def reference(w_gate, w_up, w_down, x_norm, x_act, dy_gate, dy_up, dy_down, r_gate, c_gate, r_up, c_up, r_down, c_down, hyper_params):
    new_gate, r_gate_new, c_gate_new = factored_step(w_gate, weight_grad(x_norm, dy_gate), r_gate, c_gate, hyper_params)
    new_up, r_up_new, c_up_new = factored_step(w_up, weight_grad(x_norm, dy_up), r_up, c_up, hyper_params)
    new_down, r_down_new, c_down_new = factored_step(w_down, weight_grad(x_act, dy_down), r_down, c_down, hyper_params)
    dx_norm = (input_grad(dy_gate, w_gate) + input_grad(dy_up, w_up)).astype(jnp.bfloat16)
    dx_act = input_grad(dy_down, w_down).astype(jnp.bfloat16)
    return (new_gate, new_up, new_down, r_gate_new, c_gate_new, r_up_new, c_up_new, r_down_new, c_down_new, dx_norm, dx_act)
```

```python
import functools

import jax
import jax.numpy as jnp
from jax import lax
from jax.experimental import pallas as pl
from jax.experimental.pallas import tpu as pltpu
from jax.sharding import PartitionSpec as P

EPS_ONE = 1e-30
EPS_TWO = 1e-3
CHUNKS = 16
NZ = 4
NR = 8
HOME_LAG = (3, 2, 2, 3)
F32 = jnp.float32
BF16 = jnp.bfloat16


def mm(a, b):
    return lax.dot_general(a, b, (((1,), (0,)), ((), ())), preferred_element_type=F32)


def mm_nt(a, b):
    return lax.dot_general(a, b, (((1,), (1,)), ((), ())), preferred_element_type=F32)


def mm_tn(a, b):
    return lax.dot_general(a, b, (((0,), (0,)), ((), ())), preferred_element_type=F32)


def kernel(
    xt, xa, dyg, dyu, dydt, wg, wu, wdt,
    outt, oact, gg, gu, gdt,
    rsu, rsd, ag, dz, dxy, wall, part, txt, txa, tg, tu, td, dloc, st,
    tile_sem, dloc_sem, rsu_r, rsd_r, ag_r, dz_r, dxy_r, w_r, wp_r,
    rsu_s, rsd_s, agu_s, agd_s, dzu_s, dzd_s, dxy_s, w_s, wp_s, wl_s,
    out_sem, st_l, st_s, oact_r,
):
    z = lax.axis_index("col")
    i = lax.axis_index("row")
    core = i % 2
    xx = (i // 2) % 2
    yy = i // 4
    base = z * NR
    partner = i + 1 - 2 * core
    xn = i + 2 * (1 - 2 * xx)
    yn = i + 4 * (1 - 2 * yy)
    dg = xn + 4 * (1 - 2 * yy)
    plane_peers = (xn, yn, dg)
    C = rsu.shape[1]
    S = rsu.shape[3]
    Sd = dz.shape[3]
    T = xa.shape[0]
    home_len = T // NZ
    eighth = T // NR
    up_id = base + NR + i
    dn_id = base - NR + i

    def rcopy(src, dst, ssem, rsem, dev):
        return pltpu.make_async_remote_copy(
            src, dst, ssem, rsem, device_id=dev, device_id_type=pl.DeviceIdType.LOGICAL
        )

    barrier = pltpu.get_barrier_semaphore()
    peers = [base + q for q in plane_peers] + [base + partner]
    peers += [((z + d) % NZ) * NR + i for d in (1, 2, 3)]
    for dev in peers:
        pl.semaphore_signal(barrier, inc=1, device_id=dev, device_id_type=pl.DeviceIdType.LOGICAL)

    def order(j):
        odd = j % 2
        return (1 - odd) * (3 - j // 2) + odd * (j // 2)

    def tile_at(k, j):
        h = order(j)
        lag = jnp.where(h > z, z, jnp.where(h < z, NZ - 1 - z, jnp.maximum(z, NZ - 1 - z)))
        c = k - lag
        return h, c, jnp.logical_and(c >= 0, c < C)

    def tile_copies(h, c, slot):
        t0 = pl.multiple_of(h * home_len + c * S, S)
        rows = pl.ds(t0, S)
        return [
            pltpu.make_async_copy(xt.at[:, rows], txt.at[slot], tile_sem.at[slot, 0]),
            pltpu.make_async_copy(xa.at[rows, :], txa.at[slot], tile_sem.at[slot, 1]),
            pltpu.make_async_copy(dyg.at[rows, :], tg.at[slot], tile_sem.at[slot, 2]),
            pltpu.make_async_copy(dyu.at[rows, :], tu.at[slot], tile_sem.at[slot, 3]),
            pltpu.make_async_copy(dydt.at[:, rows], td.at[slot], tile_sem.at[slot, 4]),
        ]

    def start_tile(k, j, slot):
        h, c, on = tile_at(k, j)

        @pl.when(on)
        def _():
            for cp in tile_copies(h, c, slot):
                cp.start()

    def dloc_copies(c, slot):
        return [
            pltpu.make_async_copy(
                dydt.at[:, pl.ds(pl.multiple_of(q * eighth + c * Sd, Sd), Sd)],
                dloc.at[slot, s], dloc_sem.at[slot, s])
            for s, q in enumerate((i,) + plane_peers)
        ]

    def st_local(c, slot):
        return [
            pltpu.make_async_copy(
                st.at[slot, 0, s],
                oact.at[pl.ds(pl.multiple_of(q * eighth + c * Sd, Sd), Sd), :],
                st_l.at[slot, s])
            for s, q in enumerate((i,) + plane_peers)
        ]

    def st_remote(c, slot):
        return [
            rcopy(
                st.at[slot, 1, s],
                oact.at[pl.ds(pl.multiple_of(q * eighth + c * Sd, Sd), Sd), :],
                st_s.at[slot, s], oact_r.at[0], base + partner)
            for s, q in enumerate((i,) + plane_peers)
        ]

    def out_copy(h, c):
        return pltpu.make_async_copy(
            ag.at[h, c], outt.at[:, pl.ds(pl.multiple_of(h * home_len + c * S, S), S)], out_sem.at[0])

    def w_copy(d):
        return rcopy(wdt, wall.at[0, NZ - d], w_s.at[d - 1], w_r.at[NZ - d - 1], ((z + d) % NZ) * NR + i)

    wp_copy = rcopy(wall.at[0], wall.at[1], wp_s.at[0], wp_r.at[0], base + partner)

    start_tile(0, 0, 0)
    gg[...] = jnp.zeros_like(gg)
    gu[...] = jnp.zeros_like(gu)
    gdt[...] = jnp.zeros_like(gdt)
    wl = pltpu.make_async_copy(wdt, wall.at[0, 0], wl_s.at[0])
    wl.start()
    wl.wait()
    pl.semaphore_wait(barrier, len(peers))
    for d in (1, 2, 3):
        w_copy(d).start()

    def step(k, carry):
        @pl.when(k < C)
        def _():
            src = dydt.at[:, pl.ds(pl.multiple_of(i * eighth + k * Sd, Sd), Sd)]

            @pl.when(z < NZ - 1)
            def _():
                rcopy(src, dz.at[k, 2], dzu_s.at[0], dz_r.at[2, k], up_id).start()

            @pl.when(z > 0)
            def _():
                rcopy(src, dz.at[k, 0], dzd_s.at[0], dz_r.at[0, k], dn_id).start()

        for d in (1, 2, 3):
            c = k - d
            ok = jnp.logical_and(c >= 0, c < C)

            @pl.when(jnp.logical_and(ok, z >= d))
            def _():
                rcopy(dz.at[c, 3 - d], dz.at[c, 3 - d], dzu_s.at[0], dz_r.at[3 - d, c], up_id).wait_recv()
                if d < 3:
                    @pl.when(z < NZ - 1)
                    def _():
                        rcopy(dz.at[c, 3 - d], dz.at[c, 2 - d], dzu_s.at[d], dz_r.at[2 - d, c], up_id).start()

            @pl.when(jnp.logical_and(ok, NZ - 1 - z >= d))
            def _():
                rcopy(dz.at[c, d - 1], dz.at[c, d - 1], dzd_s.at[0], dz_r.at[d - 1, c], dn_id).wait_recv()
                if d < 3:
                    @pl.when(z > 0)
                    def _():
                        rcopy(dz.at[c, d - 1], dz.at[c, d], dzd_s.at[d], dz_r.at[d, c], dn_id).start()

        cx = k - 3

        @pl.when(jnp.logical_and(cx >= 0, cx < C))
        def _():
            for s, q in enumerate(plane_peers):
                rcopy(dz.at[cx], dxy.at[s, cx], dxy_s.at[s], dxy_r.at[s, cx], base + q).start()

        for h in range(NZ):
            dist = jnp.abs(z - h)
            c = k - HOME_LAG[h] - dist

            @pl.when(jnp.logical_and(jnp.logical_and(c >= 0, c < C), z != h))
            def _():
                rcopy(ag.at[h, c], ag.at[h, c], agu_s.at[h], ag_r.at[h, c], up_id).wait_recv()

                if h < NZ - 2:
                    @pl.when(jnp.logical_and(z > h, z < NZ - 1))
                    def _():
                        rcopy(ag.at[h, c], ag.at[h, c], agu_s.at[h], ag_r.at[h, c], up_id).start()

                if h > 1:
                    @pl.when(jnp.logical_and(z < h, z > 0))
                    def _():
                        rcopy(ag.at[h, c], ag.at[h, c], agd_s.at[h], ag_r.at[h, c], dn_id).start()

                out_copy(h, c).start()

        def tile(j, carry2):
            slot = j % 2
            nj = j + 1
            start_tile(k + nj // 4, nj % 4, nj % 2)
            h, c, on = tile_at(k, j)

            @pl.when(on)
            def _():
                for cp in tile_copies(h, c, slot):
                    cp.wait()
                g = tg[slot]
                u = tu[slot]
                part[...] = mm_nt(wg[...], g) + mm_nt(wu[...], u)

                @pl.when(h > z)
                def _():
                    @pl.when(z > 0)
                    def _():
                        rcopy(rsu.at[h - 1, c], rsu.at[h - 1, c], rsu_s.at[h - 1], rsu_r.at[h - 1, c], up_id).wait_recv()
                        rsu[h - 1, c] = rsu[h - 1, c] + part[...]

                    @pl.when(z == 0)
                    def _():
                        rsu[h - 1, c] = part[...]

                    rcopy(rsu.at[h - 1, c], rsu.at[h - 1, c], rsu_s.at[h - 1], rsu_r.at[h - 1, c], up_id).start()

                @pl.when(h < z)
                def _():
                    @pl.when(z < NZ - 1)
                    def _():
                        rcopy(rsd.at[h, c], rsd.at[h, c], rsd_s.at[h], rsd_r.at[h, c], dn_id).wait_recv()
                        rsd[h, c] = rsd[h, c] + part[...]

                    @pl.when(z == NZ - 1)
                    def _():
                        rsd[h, c] = part[...]

                    rcopy(rsd.at[h, c], rsd.at[h, c], rsd_s.at[h], rsd_r.at[h, c], dn_id).start()

                @pl.when(h == z)
                def _():
                    @pl.when(z > 0)
                    def _():
                        rcopy(rsu.at[h - 1, c], rsu.at[h - 1, c], rsu_s.at[h - 1], rsu_r.at[h - 1, c], up_id).wait_recv()
                        part[...] = part[...] + rsu[h - 1, c]

                    @pl.when(z < NZ - 1)
                    def _():
                        rcopy(rsd.at[h, c], rsd.at[h, c], rsd_s.at[h], rsd_r.at[h, c], dn_id).wait_recv()
                        part[...] = part[...] + rsd[h, c]

                    ag[h, c] = part[...].astype(BF16)

                    @pl.when(z < NZ - 1)
                    def _():
                        rcopy(ag.at[h, c], ag.at[h, c], agu_s.at[h], ag_r.at[h, c], up_id).start()

                    @pl.when(z > 0)
                    def _():
                        rcopy(ag.at[h, c], ag.at[h, c], agd_s.at[h], ag_r.at[h, c], dn_id).start()

                    out_copy(h, c).start()

                gg[...] += mm(txt[slot], g)
                gu[...] += mm(txt[slot], u)
                gdt[...] += mm(td[slot], txa[slot])

            return carry2

        lax.fori_loop(0, 4, tile, 0)

        @pl.when(k == 1)
        def _():
            for d in (1, 2, 3):
                w_copy(NZ - d).wait_send()
                rcopy(wdt, wall.at[0, d], w_s.at[d - 1], w_r.at[d - 1], up_id).wait_recv()
            wp_copy.start()

        @pl.when(k == 3)
        def _():
            wp_copy.wait()

        cf = k - 4

        @pl.when(jnp.logical_and(cf >= 0, cf < C))
        def _():
            for cp in dloc_copies(cf, cf % 2):
                cp.start()

        ca = k - 5
        slot_a = ca % 2

        @pl.when(jnp.logical_and(ca >= 0, ca < C))
        def _():
            @pl.when(ca >= 2)
            def _():
                for cp in st_local(ca - 2, slot_a):
                    cp.wait()
                for cp in st_remote(ca - 2, slot_a):
                    cp.wait_send()

            locs = dloc_copies(ca, slot_a)
            outl = st_local(ca, slot_a)
            outr = st_remote(ca, slot_a)
            for s in range(4):
                locs[s].wait()
                if s == 0:
                    far = dz[ca]
                else:
                    rcopy(dz.at[ca], dxy.at[s - 1, ca], dxy_s.at[s - 1], dxy_r.at[s - 1, ca], base + xn).wait_recv()
                    far = dxy[s - 1, ca]
                lhs = jnp.concatenate([dloc[slot_a, s], far.reshape(3 * far.shape[1], Sd)], axis=0)
                for b in range(2):
                    w = wall[b].reshape(lhs.shape[0], wall.shape[3])
                    st[slot_a, b, s] = mm_tn(lhs, w).astype(BF16)
                outl[s].start()
                outr[s].start()

        return carry

    lax.fori_loop(0, C + 6, step, 0)

    for c in (C - 2, C - 1):
        for cp in st_local(c, c % 2):
            cp.wait()
        for cp in st_remote(c, c % 2):
            cp.wait_send()
    half = oact.at[pl.ds(0, T // 2), :]
    rcopy(half, half, st_s.at[0, 0], oact_r.at[0], base + partner).wait_recv()
    pltpu.make_async_copy(outt, outt, out_sem.at[0]).wait()
    for h in (1, 2, 3):
        @pl.when(h > z)
        def _():
            rcopy(rsu.at[h - 1], rsu.at[h - 1], rsu_s.at[h - 1], rsu_r.at[h - 1, 0], up_id).wait_send()
    for h in (0, 1, 2):
        @pl.when(h < z)
        def _():
            rcopy(rsd.at[h], rsd.at[h], rsd_s.at[h], rsd_r.at[h, 0], dn_id).wait_send()
    for h in range(NZ):
        if h < NZ - 1:
            @pl.when(jnp.logical_and(z >= h, z < NZ - 1))
            def _():
                rcopy(ag.at[h], ag.at[h], agu_s.at[h], ag_r.at[h, 0], up_id).wait_send()
        if h > 0:
            @pl.when(jnp.logical_and(z <= h, z > 0))
            def _():
                rcopy(ag.at[h], ag.at[h], agd_s.at[h], ag_r.at[h, 0], dn_id).wait_send()
    dzall = dxy.at[0, :, 0]
    for d in range(3):
        @pl.when(jnp.logical_and(z >= d, z < NZ - 1))
        def _():
            rcopy(dzall, dzall, dzu_s.at[d], dz_r.at[0, 0], up_id).wait_send()

        @pl.when(jnp.logical_and(NZ - 1 - z >= d, z > 0))
        def _():
            rcopy(dzall, dzall, dzd_s.at[d], dz_r.at[0, 0], dn_id).wait_send()
    for s in range(3):
        rcopy(dz, dxy.at[s], dxy_s.at[s], dxy_r.at[s, 0], base + xn).wait_send()


def main_call(xt, xa, dyg, dyu, dydt, wg, wu, wdt):
    T, ka = xa.shape
    m = xt.shape[0]
    n = dyg.shape[1]
    nd = dydt.shape[0]
    C = CHUNKS
    S = T // NZ // C
    Sd = T // NR // C
    dma = pltpu.SemaphoreType.DMA
    anyspec = pl.BlockSpec(memory_space=pl.ANY)
    vspec = pl.BlockSpec(memory_space=pltpu.VMEM)
    scratch = [
        pltpu.VMEM((3, C, m, S), F32),
        pltpu.VMEM((3, C, m, S), F32),
        pltpu.VMEM((NZ, C, m, S), BF16),
        pltpu.VMEM((C, 3, nd, Sd), BF16),
        pltpu.VMEM((3, C, 3, nd, Sd), BF16),
        pltpu.VMEM((2, NZ, nd, ka), BF16),
        pltpu.VMEM((m, S), F32),
        pltpu.VMEM((2, m, S), BF16),
        pltpu.VMEM((2, S, ka), BF16),
        pltpu.VMEM((2, S, n), BF16),
        pltpu.VMEM((2, S, n), BF16),
        pltpu.VMEM((2, nd, S), BF16),
        pltpu.VMEM((2, 4, nd, Sd), BF16),
        pltpu.VMEM((2, 2, 4, Sd, ka), BF16),
        dma((2, 5)), dma((2, 4)),
        dma((3, C)), dma((3, C)), dma((NZ, C)), dma((3, C)), dma((3, C)), dma((3,)), dma((1,)),
        dma((3,)), dma((3,)), dma((NZ,)), dma((NZ,)), dma((3,)), dma((3,)), dma((3,)), dma((3,)), dma((1,)), dma((1,)),
        dma((1,)), dma((2, 4)), dma((2, 4)), dma((1,)),
    ]
    return pl.pallas_call(
        kernel,
        out_shape=(
            jax.ShapeDtypeStruct((m, T), BF16),
            jax.ShapeDtypeStruct((T, ka), BF16),
            jax.ShapeDtypeStruct((m, n), F32),
            jax.ShapeDtypeStruct((m, n), F32),
            jax.ShapeDtypeStruct((nd, ka), F32),
        ),
        in_specs=[anyspec] * 5 + [vspec] * 3,
        out_specs=(anyspec, anyspec, vspec, vspec, vspec),
        scratch_shapes=scratch,
        compiler_params=pltpu.CompilerParams(
            collective_id=0, has_side_effects=True, vmem_limit_bytes=67_000_000),
    )(xt, xa, dyg, dyu, dydt, wg, wu, wdt)


def factored_step(w_loc, grad_loc, r_loc, c_loc, hyper_params, m_total, n_total):
    beta_two = hyper_params[0]
    grad_sq = grad_loc * grad_loc + EPS_ONE
    row_sum = lax.psum(jnp.sum(grad_sq, axis=1), 'col')
    col_sum = lax.psum(jnp.sum(grad_sq, axis=0), 'row')
    r_new = beta_two * r_loc + (1.0 - beta_two) * (row_sum / n_total)
    c_new = beta_two * c_loc + (1.0 - beta_two) * (col_sum / m_total)
    r_mean = lax.psum(jnp.sum(r_new), 'row') / m_total
    update = grad_loc * lax.rsqrt(r_new[:, None] * c_new[None, :] / r_mean)
    u_sq = lax.psum(jnp.sum(update * update), ('row', 'col'))
    rms_u = jnp.sqrt(u_sq / (m_total * n_total))
    update_hat = update / jnp.maximum(1.0, rms_u / hyper_params[2])
    w_sq = lax.psum(jnp.sum(w_loc * w_loc), ('row', 'col'))
    step_size = hyper_params[1] * jnp.maximum(EPS_TWO, jnp.sqrt(w_sq / (m_total * n_total)))
    return w_loc - step_size * update_hat, r_new, c_new


def solution(mesh):
    row_size = mesh.shape['row']
    col_size = mesh.shape['col']
    weight_spec = P('row', 'col')
    act_spec = P(None, 'row')
    grad_spec = P(None, 'col')
    in_specs = (weight_spec,) * 3 + (act_spec, act_spec) + (grad_spec,) * 3 + (P('row'), P('col')) * 3 + (P(),)
    out_specs = (weight_spec,) * 3 + (P('row'), P('col')) * 3 + (act_spec, act_spec)

    def body(w_gate, w_up, w_down, x_norm, x_act, dy_gate, dy_up, dy_down, r_gate, c_gate, r_up, c_up, r_down, c_down, hyper_params):
        d_model = w_gate.shape[0] * row_size
        d_ff = w_gate.shape[1] * col_size
        outt, dx_act, g_gate, g_up, g_down_t = main_call(
            x_norm.T, x_act, dy_gate, dy_up, dy_down.T,
            w_gate.astype(BF16), w_up.astype(BF16), w_down.T.astype(BF16))
        new_gate, r_gate_new, c_gate_new = factored_step(w_gate, g_gate, r_gate, c_gate, hyper_params, d_model, d_ff)
        new_up, r_up_new, c_up_new = factored_step(w_up, g_up, r_up, c_up, hyper_params, d_model, d_ff)
        new_down, r_down_new, c_down_new = factored_step(w_down, g_down_t.T, r_down, c_down, hyper_params, d_ff, d_model)
        return (new_gate, new_up, new_down, r_gate_new, c_gate_new, r_up_new, c_up_new, r_down_new, c_down_new, outt.T, dx_act)

    return jax.shard_map(body, mesh=mesh, in_specs=in_specs, out_specs=out_specs, check_vma=False)
```

```python
import jax
import jax.numpy as jnp
from jax import lax
from jax.experimental import pallas as pl
from jax.experimental.pallas import tpu as pltpu
from jax.sharding import PartitionSpec as P

EPS_ONE = 1e-30
EPS_TWO = 1e-3
CHUNKS = 32
NZ = 4
NR = 8
HOME_LAG = (3, 2, 2, 3)
F32 = jnp.float32
BF16 = jnp.bfloat16


def mm(a, b):
    return lax.dot_general(a, b, (((1,), (0,)), ((), ())), preferred_element_type=F32)


def mm_nt(a, b):
    return lax.dot_general(a, b, (((1,), (1,)), ((), ())), preferred_element_type=F32)


def mm_tn(a, b):
    return lax.dot_general(a, b, (((0,), (0,)), ((), ())), preferred_element_type=F32)


def kernel(
    xt, xa, dyg, dyu, dydt, wgf, wuf, wdf, rg, cg, ru, cu, rd, cd, hp,
    outt, oact, gg, gu, gdt, sv,
    rsu, rsd, ag, dz, dxy, wall, part, txt, txa, tg, tu, td, dloc, st,
    wg, wu, wdt, sa, sb, s1, s2,
    tile_sem, dloc_sem, rsu_r, rsd_r, ag_r, dz_r, dxy_r, w_r, wp_r,
    rsu_s, rsd_s, agu_s, agd_s, dzu_s, dzd_s, dxy_s, wu_s, wd_s, wp_s,
    out_sem, st_l, st_s, oact_r, small_s, small_r,
):
    z = lax.axis_index("col")
    i = lax.axis_index("row")
    core = i % 2
    xx = (i // 2) % 2
    yy = i // 4
    base = z * NR
    partner = i + 1 - 2 * core
    xn = i + 2 * (1 - 2 * xx)
    yn = i + 4 * (1 - 2 * yy)
    dg = xn + 4 * (1 - 2 * yy)
    plane_peers = (xn, yn, dg)
    C = rsu.shape[1]
    S = rsu.shape[3]
    Sd = dz.shape[3]
    T = xa.shape[0]
    home_len = T // NZ
    eighth = T // NR
    up_id = base + NR + i
    dn_id = base - NR + i

    def rcopy(src, dst, ssem, rsem, dev):
        return pltpu.make_async_remote_copy(
            src, dst, ssem, rsem, device_id=dev, device_id_type=pl.DeviceIdType.LOGICAL
        )

    barrier = pltpu.get_barrier_semaphore()
    me = base + i
    ndev = NZ * NR

    def greet(d, carry):
        pl.semaphore_signal(barrier, inc=1, device_id=(me + d) % ndev, device_id_type=pl.DeviceIdType.LOGICAL)
        return carry

    lax.fori_loop(1, ndev, greet, 0)

    def tile_copies(h, c, slot):
        t0 = pl.multiple_of(h * home_len + c * S, S)
        rows = pl.ds(t0, S)
        return [
            pltpu.make_async_copy(xt.at[:, rows], txt.at[slot], tile_sem.at[slot, 0]),
            pltpu.make_async_copy(xa.at[rows, :], txa.at[slot], tile_sem.at[slot, 1]),
            pltpu.make_async_copy(dyg.at[rows, :], tg.at[slot], tile_sem.at[slot, 2]),
            pltpu.make_async_copy(dyu.at[rows, :], tu.at[slot], tile_sem.at[slot, 3]),
            pltpu.make_async_copy(dydt.at[:, rows], td.at[slot], tile_sem.at[slot, 4]),
        ]

    def start_tile(h, c, slot):
        @pl.when(c < C)
        def _():
            for cp in tile_copies(h, c, slot):
                cp.start()

    def dloc_copies(c, slot):
        return [
            pltpu.make_async_copy(
                dydt.at[:, pl.ds(pl.multiple_of(q * eighth + c * Sd, Sd), Sd)],
                dloc.at[slot, s], dloc_sem.at[slot, s])
            for s, q in enumerate((i,) + plane_peers)
        ]

    def st_local(c, slot):
        return [
            pltpu.make_async_copy(
                st.at[slot, 0, s],
                oact.at[pl.ds(pl.multiple_of(q * eighth + c * Sd, Sd), Sd), :],
                st_l.at[slot, s])
            for s, q in enumerate((i,) + plane_peers)
        ]

    def st_remote(c, slot):
        return [
            rcopy(
                st.at[slot, 1, s],
                oact.at[pl.ds(pl.multiple_of(q * eighth + c * Sd, Sd), Sd), :],
                st_s.at[slot, s], oact_r.at[0], base + partner)
            for s, q in enumerate((i,) + plane_peers)
        ]

    def out_copy(h, c):
        return pltpu.make_async_copy(
            ag.at[h, c], outt.at[:, pl.ds(pl.multiple_of(h * home_len + c * S, S), S)], out_sem.at[0])

    wp_copy = rcopy(wall.at[0], wall.at[1], wp_s.at[0], wp_r.at[0], base + partner)

    def scalar_copy(ref, t, d):
        return rcopy(ref.at[me], ref.at[me], small_s.at[t], small_r.at[t], (me + d) % ndev)

    def row_copy(d):
        return rcopy(sa.at[i], sa.at[i], small_s.at[0], small_r.at[0], base + (i + d) % NR)

    def col_copy(d):
        return rcopy(sb.at[z], sb.at[z], small_s.at[1], small_r.at[1], ((z + d) % NZ) * NR + i)

    def lanes_of(v, width):
        n = v.shape[0]
        r_id = lax.broadcasted_iota(jnp.int32, (n, width), 0)
        l_id = lax.broadcasted_iota(jnp.int32, (n, width), 1)
        return jnp.sum(jnp.where(r_id == l_id, v, 0.0), axis=0, keepdims=True)

    def column_of(v, n):
        width = v.shape[1]
        r_id = lax.broadcasted_iota(jnp.int32, (n, width), 0)
        l_id = lax.broadcasted_iota(jnp.int32, (n, width), 1)
        return jnp.sum(jnp.where(r_id == l_id, v, 0.0), axis=1, keepdims=True)

    def total(v):
        return jnp.sum(jnp.sum(v, axis=1, keepdims=True), axis=0, keepdims=True)

    def pack_lanes(vals):
        lane = lax.broadcasted_iota(jnp.int32, (1, 128), 1)
        out = jnp.zeros((1, 128), F32)
        for t, v in enumerate(vals):
            out = jnp.where(lane == t, v, out)
        return out

    def lane_value(v, t):
        lane = lax.broadcasted_iota(jnp.int32, (1, 128), 1)
        return jnp.sum(jnp.where(lane == t, v, 0.0), axis=1, keepdims=True)

    m_gu = NR * gg.shape[0]
    n_gu = NZ * gg.shape[1]
    m_dn = NR * gdt.shape[1]
    n_dn = NZ * gdt.shape[0]
    mg = gg.shape[0]
    ng = gg.shape[1]
    md = gdt.shape[1]
    nd = gdt.shape[0]
    beta = hp[0]
    rho = hp[1]
    dcut = hp[2]

    def first_sums():
        tot = []
        for t, ref in enumerate((gg, gu)):
            g = ref[...]
            q = g * g + EPS_ONE
            rows = jnp.sum(q, axis=1, keepdims=True)
            sa[i, t] = jnp.sum(q, axis=0, keepdims=True)
            sb[z, t, :, pl.ds(0, 128)] = lanes_of(rows, 128)
            tot.append(total(rows))
        g = gdt[...]
        q = g * g + EPS_ONE
        n_sum = jnp.sum(q, axis=1, keepdims=True)
        sa[i, 2, :, pl.ds(0, 256)] = lanes_of(n_sum, 256)
        sb[z, 2] = jnp.sum(q, axis=0, keepdims=True)
        tot.append(total(n_sum))
        for ref in (wgf, wuf, wdf):
            w = ref[...]
            tot.append(total(w * w))
        for ref in (rg, ru, rd):
            tot.append(total(ref[...]))
        s1[me] = pack_lanes(tot)
        for d in range(1, NR):
            row_copy(d).start()
        for d in range(1, NZ):
            col_copy(d).start()

        def send(d, carry):
            scalar_copy(s1, 2, d).start()
            return carry

        lax.fori_loop(1, ndev, send, 0)

    def second_sums():
        some = sa.at[pl.ds(0, NR - 1)]
        rcopy(some, some, small_s.at[0], small_r.at[0], base + partner).wait_recv()
        some = sb.at[pl.ds(0, NZ - 1)]
        rcopy(some, some, small_s.at[1], small_r.at[1], base + partner).wait_recv()
        some = s1.at[pl.ds(0, ndev - 1)]
        rcopy(some, some, small_s.at[2], small_r.at[2], base + partner).wait_recv()
        tot = jnp.sum(s1[...], axis=0)
        asum = jnp.sum(sa[...], axis=0)
        bsum = jnp.sum(sb[...], axis=0)
        u_sq = []
        for t, (gref, rref, cref) in enumerate(((gg, rg, cg), (gu, ru, cu))):
            r_new = beta * rref[...] + (1.0 - beta) * (bsum[t][:, :mg] / n_gu)
            c_new = beta * cref[...] + (1.0 - beta) * (asum[t] / m_gu)
            q_mean = lane_value(tot, t) / (m_gu * n_gu)
            r_mean = beta * (lane_value(tot, 6 + t) / (NZ * m_gu)) + (1.0 - beta) * q_mean
            sv[pl.ds(2 * t, 1), pl.ds(0, mg)] = r_new
            sv[pl.ds(2 * t + 1, 1), :] = c_new
            u = gref[...] * lax.rsqrt(column_of(r_new, mg) * c_new / r_mean)
            gref[...] = u
            u_sq.append(total(u * u))
        r_new = beta * rd[...] + (1.0 - beta) * (bsum[2] / n_dn)
        c_new = beta * cd[...] + (1.0 - beta) * (asum[2][:, :nd] / m_dn)
        q_mean = lane_value(tot, 2) / (m_dn * n_dn)
        r_mean = beta * (lane_value(tot, 8) / (NZ * m_dn)) + (1.0 - beta) * q_mean
        sv[pl.ds(4, 1), pl.ds(0, md)] = r_new
        sv[pl.ds(5, 1), pl.ds(0, nd)] = c_new
        u = gdt[...] * lax.rsqrt(r_new * column_of(c_new, nd) / r_mean)
        gdt[...] = u
        u_sq.append(total(u * u))
        s2[me] = pack_lanes(u_sq)

        def send(d, carry):
            scalar_copy(s2, 3, d).start()
            return carry

        lax.fori_loop(1, ndev, send, 0)
        size = m_gu * n_gu
        sv[pl.ds(6, 1), pl.ds(0, 128)] = pack_lanes(
            [rho * jnp.maximum(EPS_TWO, jnp.sqrt(lane_value(tot, 3 + t) / size)) for t in range(3)])

    def third_sums():
        some = s2.at[pl.ds(0, ndev - 1)]
        rcopy(some, some, small_s.at[3], small_r.at[3], base + partner).wait_recv()
        rms_u = jnp.sqrt(jnp.sum(s2[...], axis=0) / (m_gu * n_gu))
        sv[pl.ds(7, 1), pl.ds(0, 128)] = sv[pl.ds(6, 1), pl.ds(0, 128)] / jnp.maximum(1.0, rms_u / dcut)

    for t, h in ((0, 3), (1, 0)):
        start_tile(h, 0, t)
    gg[...] = jnp.zeros_like(gg)
    gu[...] = jnp.zeros_like(gu)
    gdt[...] = jnp.zeros_like(gdt)
    sa[...] = jnp.zeros_like(sa)
    sb[...] = jnp.zeros_like(sb)
    sv[...] = jnp.zeros_like(sv)
    wg[...] = wgf[...].astype(BF16)
    wu[...] = wuf[...].astype(BF16)
    wdt[...] = wdf[...].astype(BF16)
    wall[0, 0] = wdt[...]
    pl.semaphore_wait(barrier, ndev - 1)

    @pl.when(z < NZ - 1)
    def _():
        rcopy(wdt, wall.at[0, 3], wu_s.at[0], w_r.at[2], up_id).start()

    @pl.when(z > 0)
    def _():
        rcopy(wdt, wall.at[0, 1], wd_s.at[0], w_r.at[0], dn_id).start()

    def step(k, carry):
        @pl.when(k < C)
        def _():
            src = dydt.at[:, pl.ds(pl.multiple_of(i * eighth + k * Sd, Sd), Sd)]

            @pl.when(z < NZ - 1)
            def _():
                rcopy(src, dz.at[k, 2], dzu_s.at[0], dz_r.at[2, k], up_id).start()

            @pl.when(z > 0)
            def _():
                rcopy(src, dz.at[k, 0], dzd_s.at[0], dz_r.at[0, k], dn_id).start()

        for d in (1, 2, 3):
            c = k - d
            ok = jnp.logical_and(c >= 0, c < C)

            @pl.when(jnp.logical_and(k == d, z >= d))
            def _():
                rcopy(wdt, wall.at[0, 4 - d], wu_s.at[0], w_r.at[3 - d], up_id).wait_recv()
                if d < 3:
                    @pl.when(z < NZ - 1)
                    def _():
                        rcopy(wall.at[0, 4 - d], wall.at[0, 3 - d], wu_s.at[d], w_r.at[2 - d], up_id).start()

            @pl.when(jnp.logical_and(k == d, NZ - 1 - z >= d))
            def _():
                rcopy(wdt, wall.at[0, d], wd_s.at[0], w_r.at[d - 1], dn_id).wait_recv()
                if d < 3:
                    @pl.when(z > 0)
                    def _():
                        rcopy(wall.at[0, d], wall.at[0, d + 1], wd_s.at[d], w_r.at[d], dn_id).start()

            @pl.when(jnp.logical_and(ok, z >= d))
            def _():
                rcopy(dz.at[c, 3 - d], dz.at[c, 3 - d], dzu_s.at[0], dz_r.at[3 - d, c], up_id).wait_recv()
                if d < 3:
                    @pl.when(z < NZ - 1)
                    def _():
                        rcopy(dz.at[c, 3 - d], dz.at[c, 2 - d], dzu_s.at[d], dz_r.at[2 - d, c], up_id).start()

            @pl.when(jnp.logical_and(ok, NZ - 1 - z >= d))
            def _():
                rcopy(dz.at[c, d - 1], dz.at[c, d - 1], dzd_s.at[0], dz_r.at[d - 1, c], dn_id).wait_recv()
                if d < 3:
                    @pl.when(z > 0)
                    def _():
                        rcopy(dz.at[c, d - 1], dz.at[c, d], dzd_s.at[d], dz_r.at[d, c], dn_id).start()

        cx = k - 3

        @pl.when(jnp.logical_and(cx >= 0, cx < C))
        def _():
            for s, q in enumerate(plane_peers):
                rcopy(dz.at[cx], dxy.at[s, cx], dxy_s.at[s], dxy_r.at[s, cx], base + q).start()

        for h in range(NZ):
            dist = jnp.abs(z - h)
            c = k - HOME_LAG[h] - dist

            @pl.when(jnp.logical_and(jnp.logical_and(c >= 0, c < C), z != h))
            def _():
                rcopy(ag.at[h, c], ag.at[h, c], agu_s.at[h], ag_r.at[h, c], up_id).wait_recv()

                if h < NZ - 2:
                    @pl.when(jnp.logical_and(z > h, z < NZ - 1))
                    def _():
                        rcopy(ag.at[h, c], ag.at[h, c], agu_s.at[h], ag_r.at[h, c], up_id).start()

                if h > 1:
                    @pl.when(jnp.logical_and(z < h, z > 0))
                    def _():
                        rcopy(ag.at[h, c], ag.at[h, c], agd_s.at[h], ag_r.at[h, c], dn_id).start()

                out_copy(h, c).start()

        @pl.when(k == C)
        def _():
            first_sums()

        @pl.when(k == C + 2)
        def _():
            second_sums()

        @pl.when(k == C + 4)
        def _():
            third_sums()

        order = (3, 0, 2, 1)
        for t, h in enumerate(order):
            slot = t % 2

            @pl.when(k < C)
            def _():
                for cp in tile_copies(h, k, slot):
                    cp.wait()
                g = tg[slot]
                u = tu[slot]
                part[k % 4, h] = mm_nt(wg[...], g) + mm_nt(wu[...], u)
                gg[...] += mm(txt[slot], g)
                gu[...] += mm(txt[slot], u)
                gdt[...] += mm(td[slot], txa[slot])

            start_tile(order[(t + 2) % 4], k + (t + 2) // 4, slot)

            if h > 0:
                c = k - z

                @pl.when(jnp.logical_and(h > z, jnp.logical_and(c >= 0, c < C)))
                def _():
                    @pl.when(z > 0)
                    def _():
                        rcopy(rsu.at[h - 1, c], rsu.at[h - 1, c], rsu_s.at[h - 1], rsu_r.at[h - 1, c], up_id).wait_recv()
                        rsu[h - 1, c] = rsu[h - 1, c] + part[c % 4, h]

                    @pl.when(z == 0)
                    def _():
                        rsu[h - 1, c] = part[c % 4, h]

                    rcopy(rsu.at[h - 1, c], rsu.at[h - 1, c], rsu_s.at[h - 1], rsu_r.at[h - 1, c], up_id).start()

            if h < NZ - 1:
                c2 = k - (NZ - 1 - z)

                @pl.when(jnp.logical_and(h < z, jnp.logical_and(c2 >= 0, c2 < C)))
                def _():
                    @pl.when(z < NZ - 1)
                    def _():
                        rcopy(rsd.at[h, c2], rsd.at[h, c2], rsd_s.at[h], rsd_r.at[h, c2], dn_id).wait_recv()
                        rsd[h, c2] = rsd[h, c2] + part[c2 % 4, h]

                    @pl.when(z == NZ - 1)
                    def _():
                        rsd[h, c2] = part[c2 % 4, h]

                    rcopy(rsd.at[h, c2], rsd.at[h, c2], rsd_s.at[h], rsd_r.at[h, c2], dn_id).start()

            c3 = k - HOME_LAG[h]

            @pl.when(jnp.logical_and(h == z, jnp.logical_and(c3 >= 0, c3 < C)))
            def _():
                acc = part[c3 % 4, h]
                if h > 0:
                    rcopy(rsu.at[h - 1, c3], rsu.at[h - 1, c3], rsu_s.at[h - 1], rsu_r.at[h - 1, c3], up_id).wait_recv()
                    acc = acc + rsu[h - 1, c3]
                if h < NZ - 1:
                    rcopy(rsd.at[h, c3], rsd.at[h, c3], rsd_s.at[h], rsd_r.at[h, c3], dn_id).wait_recv()
                    acc = acc + rsd[h, c3]
                ag[h, c3] = acc.astype(BF16)
                if h < NZ - 1:
                    rcopy(ag.at[h, c3], ag.at[h, c3], agu_s.at[h], ag_r.at[h, c3], up_id).start()
                if h > 0:
                    rcopy(ag.at[h, c3], ag.at[h, c3], agd_s.at[h], ag_r.at[h, c3], dn_id).start()
                out_copy(h, c3).start()

        @pl.when(k == 3)
        def _():
            wp_copy.start()

        @pl.when(k == 5)
        def _():
            wp_copy.wait()

        cf = k - 4

        @pl.when(jnp.logical_and(cf >= 0, cf < C))
        def _():
            for cp in dloc_copies(cf, cf % 2):
                cp.start()

        ca = k - 5
        slot_a = ca % 2

        @pl.when(jnp.logical_and(ca >= 0, ca < C))
        def _():
            @pl.when(ca >= 2)
            def _():
                for cp in st_local(ca - 2, slot_a):
                    cp.wait()
                for cp in st_remote(ca - 2, slot_a):
                    cp.wait_send()

            locs = dloc_copies(ca, slot_a)
            outl = st_local(ca, slot_a)
            outr = st_remote(ca, slot_a)
            for s in range(4):
                locs[s].wait()
                if s == 0:
                    far = dz[ca]
                else:
                    rcopy(dz.at[ca], dxy.at[s - 1, ca], dxy_s.at[s - 1], dxy_r.at[s - 1, ca], base + xn).wait_recv()
                    far = dxy[s - 1, ca]
                lhs = jnp.concatenate([dloc[slot_a, s], far.reshape(3 * far.shape[1], Sd)], axis=0)
                for b in range(2):
                    w = wall[b].reshape(lhs.shape[0], wall.shape[3])
                    st[slot_a, b, s] = mm_tn(lhs, w).astype(BF16)
                outl[s].start()
                outr[s].start()

        return carry

    lax.fori_loop(0, C + 6, step, 0)

    for c in (C - 2, C - 1):
        for cp in st_local(c, c % 2):
            cp.wait()
        for cp in st_remote(c, c % 2):
            cp.wait_send()
    half = oact.at[pl.ds(0, T // 2), :]
    rcopy(half, half, st_s.at[0, 0], oact_r.at[0], base + partner).wait_recv()
    pltpu.make_async_copy(outt, outt, out_sem.at[0]).wait()
    for h in (1, 2, 3):
        @pl.when(h > z)
        def _():
            rcopy(rsu.at[h - 1], rsu.at[h - 1], rsu_s.at[h - 1], rsu_r.at[h - 1, 0], up_id).wait_send()
    for h in (0, 1, 2):
        @pl.when(h < z)
        def _():
            rcopy(rsd.at[h], rsd.at[h], rsd_s.at[h], rsd_r.at[h, 0], dn_id).wait_send()
    for h in range(NZ):
        if h < NZ - 1:
            @pl.when(jnp.logical_and(z >= h, z < NZ - 1))
            def _():
                rcopy(ag.at[h], ag.at[h], agu_s.at[h], ag_r.at[h, 0], up_id).wait_send()
        if h > 0:
            @pl.when(jnp.logical_and(z <= h, z > 0))
            def _():
                rcopy(ag.at[h], ag.at[h], agd_s.at[h], ag_r.at[h, 0], dn_id).wait_send()
    for d in range(3):
        @pl.when(jnp.logical_and(z >= d, z < NZ - 1))
        def _():
            rcopy(wdt, wdt, wu_s.at[d], w_r.at[0], up_id).wait_send()

        @pl.when(jnp.logical_and(NZ - 1 - z >= d, z > 0))
        def _():
            rcopy(wdt, wdt, wd_s.at[d], w_r.at[0], dn_id).wait_send()
    for t, (ref, cnt) in enumerate(((sa, NR - 1), (sb, NZ - 1), (s1, ndev - 1), (s2, ndev - 1))):
        some = ref.at[pl.ds(0, cnt)]
        rcopy(some, some, small_s.at[t], small_r.at[t], base + partner).wait_send()
    dzall = dxy.at[0, :, 0]
    for d in range(3):
        @pl.when(jnp.logical_and(z >= d, z < NZ - 1))
        def _():
            rcopy(dzall, dzall, dzu_s.at[d], dz_r.at[0, 0], up_id).wait_send()

        @pl.when(jnp.logical_and(NZ - 1 - z >= d, z > 0))
        def _():
            rcopy(dzall, dzall, dzd_s.at[d], dz_r.at[0, 0], dn_id).wait_send()
    for s in range(3):
        rcopy(dz, dxy.at[s], dxy_s.at[s], dxy_r.at[s, 0], base + xn).wait_send()


def main_call(xt, xa, dyg, dyu, dydt, wg, wu, wdt, vecs, hp):
    T, ka = xa.shape
    m = xt.shape[0]
    n = dyg.shape[1]
    nd = dydt.shape[0]
    C = CHUNKS
    S = T // NZ // C
    Sd = T // NR // C
    dma = pltpu.SemaphoreType.DMA
    anyspec = pl.BlockSpec(memory_space=pl.ANY)
    vspec = pl.BlockSpec(memory_space=pltpu.VMEM)
    sspec = pl.BlockSpec(memory_space=pltpu.SMEM)
    scratch = [
        pltpu.VMEM((3, C, m, S), F32),
        pltpu.VMEM((3, C, m, S), F32),
        pltpu.VMEM((NZ, C, m, S), BF16),
        pltpu.VMEM((C, 3, nd, Sd), BF16),
        pltpu.VMEM((3, C, 3, nd, Sd), BF16),
        pltpu.VMEM((2, NZ, nd, ka), BF16),
        pltpu.VMEM((4, NZ, m, S), F32),
        pltpu.VMEM((2, m, S), BF16),
        pltpu.VMEM((2, S, ka), BF16),
        pltpu.VMEM((2, S, n), BF16),
        pltpu.VMEM((2, S, n), BF16),
        pltpu.VMEM((2, nd, S), BF16),
        pltpu.VMEM((2, 4, nd, Sd), BF16),
        pltpu.VMEM((2, 2, 4, Sd, ka), BF16),
        pltpu.VMEM((m, n), BF16),
        pltpu.VMEM((m, n), BF16),
        pltpu.VMEM((nd, ka), BF16),
        pltpu.VMEM((NR, 3, 1, n), F32),
        pltpu.VMEM((NZ, 3, 1, 256), F32),
        pltpu.VMEM((NZ * NR, 1, 128), F32),
        pltpu.VMEM((NZ * NR, 1, 128), F32),
        dma((2, 5)), dma((2, 4)),
        dma((3, C)), dma((3, C)), dma((NZ, C)), dma((3, C)), dma((3, C)), dma((3,)), dma((1,)),
        dma((3,)), dma((3,)), dma((NZ,)), dma((NZ,)), dma((3,)), dma((3,)), dma((3,)), dma((3,)), dma((3,)), dma((1,)),
        dma((1,)), dma((2, 4)), dma((2, 4)), dma((1,)), dma((4,)), dma((4,)),
    ]
    return pl.pallas_call(
        kernel,
        out_shape=(
            jax.ShapeDtypeStruct((m, T), BF16),
            jax.ShapeDtypeStruct((T, ka), BF16),
            jax.ShapeDtypeStruct((m, n), F32),
            jax.ShapeDtypeStruct((m, n), F32),
            jax.ShapeDtypeStruct((nd, ka), F32),
            jax.ShapeDtypeStruct((8, n), F32),
        ),
        in_specs=[anyspec] * 5 + [vspec] * 9 + [sspec],
        out_specs=(anyspec, anyspec, vspec, vspec, vspec, vspec),
        scratch_shapes=scratch,
        compiler_params=pltpu.CompilerParams(
            collective_id=0, has_side_effects=True, vmem_limit_bytes=67_000_000),
    )(xt, xa, dyg, dyu, dydt, wg, wu, wdt, *vecs, hp)


def final_kernel(
    outt, oact, ug, uu, ud, sv, wg, wu, wd,
    outt_o, oact_o, wg_o, wu_o, wd_o, rg_o, cg_o, ru_o, cu_o, rd_o, cd_o,
    buft, bufa, in_t, in_a, out_t, out_a,
):
    nt = buft.shape[0]
    na = bufa.shape[0]
    ht = buft.shape[1]
    ha = bufa.shape[1]
    a_in = [pltpu.make_async_copy(oact.at[pl.ds(j * ha, ha), :], bufa.at[j], in_a.at[j]) for j in range(na)]
    a_out = [pltpu.make_async_copy(bufa.at[j], oact_o.at[pl.ds(j * ha, ha), :], out_a.at[j]) for j in range(na)]
    t_in = [pltpu.make_async_copy(outt.at[pl.ds(j * ht, ht), :], buft.at[j], in_t.at[j]) for j in range(nt)]
    t_out = [pltpu.make_async_copy(buft.at[j], outt_o.at[pl.ds(j * ht, ht), :], out_t.at[j]) for j in range(nt)]
    for cp in a_in + t_in:
        cp.start()
    for t, (u, w, o) in enumerate(((ug, wg, wg_o), (uu, wu, wu_o), (ud, wd, wd_o))):
        o[...] = w[...] - sv[7:8, t:t + 1] * u[...]
    for t, o in enumerate((rg_o, cg_o, ru_o, cu_o, rd_o, cd_o)):
        o[...] = sv[t:t + 1, :o.shape[1]]
    for cin, cout in zip(a_in + t_in, a_out + t_out):
        cin.wait()
        cout.start()
    for cp in a_out + t_out:
        cp.wait()


def final_call(outt, oact, ug, uu, ud, sv, wg, wu, wd):
    m, T = outt.shape
    ka = oact.shape[1]
    n = ug.shape[1]
    nd = ud.shape[0]
    nt = m // 16
    na = 16
    dma = pltpu.SemaphoreType.DMA
    anyspec = pl.BlockSpec(memory_space=pl.ANY)
    vspec = pl.BlockSpec(memory_space=pltpu.VMEM)
    shape = jax.ShapeDtypeStruct
    return pl.pallas_call(
        final_kernel,
        out_shape=(
            shape((m, T), BF16), shape((T, ka), BF16),
            shape((m, n), F32), shape((m, n), F32), shape((nd, ka), F32),
            shape((1, m), F32), shape((1, n), F32), shape((1, m), F32), shape((1, n), F32),
            shape((1, ka), F32), shape((1, nd), F32)),
        in_specs=[anyspec] * 2 + [vspec] * 7,
        out_specs=(anyspec,) * 2 + (vspec,) * 9,
        scratch_shapes=[
            pltpu.VMEM((nt, m // nt, T), BF16), pltpu.VMEM((na, T // na, ka), BF16),
            dma((nt,)), dma((na,)), dma((nt,)), dma((na,))],
        compiler_params=pltpu.CompilerParams(vmem_limit_bytes=64_000_000),
    )(outt, oact, ug, uu, ud, sv, wg, wu, wd)


def solution(mesh):
    weight_spec = P('row', 'col')
    act_spec = P(None, 'row')
    grad_spec = P(None, 'col')
    in_specs = (weight_spec,) * 3 + (act_spec, act_spec) + (grad_spec,) * 3 + (P('row'), P('col')) * 3 + (P(),)
    out_specs = (weight_spec,) * 3 + (P('row'), P('col')) * 3 + (act_spec, act_spec)

    def body(w_gate, w_up, w_down, x_norm, x_act, dy_gate, dy_up, dy_down, r_gate, c_gate, r_up, c_up, r_down, c_down, hyper_params):
        wdt = w_down.T
        vecs = [v.reshape(1, -1) for v in (r_gate, c_gate, r_up, c_up, r_down, c_down)]
        outt, oact, ug, uu, ud, sv = main_call(
            x_norm.T, x_act, dy_gate, dy_up, dy_down.T, w_gate, w_up, wdt, vecs, hyper_params)
        outt, dx_act, new_gate, new_up, new_down_t, *stats = final_call(outt, oact, ug, uu, ud, sv, w_gate, w_up, wdt)
        stats = [v.reshape(-1) for v in stats]
        return (new_gate, new_up, new_down_t.T, *stats, outt.T, dx_act)

    return jax.shard_map(body, mesh=mesh, in_specs=in_specs, out_specs=out_specs, check_vma=False)
```

```python
import jax
import jax.numpy as jnp
from jax import lax
from jax.experimental import pallas as pl
from jax.experimental.pallas import tpu as pltpu
from jax.sharding import PartitionSpec as P

EPS_ONE = 1e-30
EPS_TWO = 1e-3
CHUNKS = 32
NZ = 4
NR = 8
HOME_LAG = (3, 2, 2, 3)
SKEW = (0, 2, 2, 0)
AHEAD = 3
SLOTS = 8
DRAIN = 6
F32 = jnp.float32
BF16 = jnp.bfloat16


def mm(a, b):
    return lax.dot_general(a, b, (((1,), (0,)), ((), ())), preferred_element_type=F32)


def mm_nt(a, b):
    return lax.dot_general(a, b, (((1,), (1,)), ((), ())), preferred_element_type=F32)


def mm_tn(a, b):
    return lax.dot_general(a, b, (((0,), (0,)), ((), ())), preferred_element_type=F32)


def kernel(
    xt, xa, dyg, dyu, dydt, wgf, wuf, wdf, rg, cg, ru, cu, rd, cd, hp,
    ag, oact, gg, gu, gdt, sv,
    rsu, rsd, dz, dxy, wall, part, txt, txa, tg, tu, td, dloc, st,
    wg, wu, wdt, sa, sb, s1, s2,
    tile_sem, dloc_sem, rsu_r, rsd_r, ag_r, dz_r, dxy_r, w_r, wp_r,
    rsu_s, rsd_s, agu_s, agd_s, dzu_s, dzd_s, dxy_s, wu_s, wd_s, wp_s,
    st_s, oact_r, small_s, small_r,
):
    z = lax.axis_index("col")
    i = lax.axis_index("row")
    core = i % 2
    xx = (i // 2) % 2
    yy = i // 4
    base = z * NR
    partner = i + 1 - 2 * core
    xn = i + 2 * (1 - 2 * xx)
    yn = i + 4 * (1 - 2 * yy)
    dg = xn + 4 * (1 - 2 * yy)
    plane_peers = (xn, yn, dg)
    C = rsu.shape[1]
    S = rsu.shape[3]
    Sd = dz.shape[3]
    T = xa.shape[0]
    home_len = T // NZ
    eighth = T // NR
    up_id = base + NR + i
    dn_id = base - NR + i

    def rcopy(src, dst, ssem, rsem, dev):
        return pltpu.make_async_remote_copy(
            src, dst, ssem, rsem, device_id=dev, device_id_type=pl.DeviceIdType.LOGICAL
        )

    def up_sum(h, c):
        return rcopy(rsu.at[h - 1, c], rsu.at[h - 1, c], rsu_s.at[h - 1], rsu_r.at[h - 1, c], up_id)

    def dn_sum(h, c):
        return rcopy(rsd.at[h, c], rsd.at[h, c], rsd_s.at[h], rsd_r.at[h, c], dn_id)

    def up_block(h, c):
        return rcopy(ag.at[h, c], ag.at[h, c], agu_s.at[h], ag_r.at[h, c], up_id)

    def dn_block(h, c):
        return rcopy(ag.at[h, c], ag.at[h, c], agd_s.at[h], ag_r.at[h, c], dn_id)

    def both(a, b):
        return jnp.logical_and(a, b)

    def valid(c):
        return both(c >= 0, c < C)

    barrier = pltpu.get_barrier_semaphore()
    me = base + i
    ndev = NZ * NR

    def greet(d, carry):
        pl.semaphore_signal(barrier, inc=1, device_id=(me + d) % ndev, device_id_type=pl.DeviceIdType.LOGICAL)
        return carry

    lax.fori_loop(1, ndev, greet, 0)

    def tile_copies(h, c, slot):
        t0 = pl.multiple_of(h * home_len + c * S, S)
        rows = pl.ds(t0, S)
        return [
            pltpu.make_async_copy(xt.at[:, rows], txt.at[slot], tile_sem.at[slot, 0]),
            pltpu.make_async_copy(xa.at[rows, :], txa.at[slot], tile_sem.at[slot, 1]),
            pltpu.make_async_copy(dyg.at[rows, :], tg.at[slot], tile_sem.at[slot, 2]),
            pltpu.make_async_copy(dyu.at[rows, :], tu.at[slot], tile_sem.at[slot, 3]),
            pltpu.make_async_copy(dydt.at[:, rows], td.at[slot], tile_sem.at[slot, 4]),
        ]

    def start_tile(h, c, slot):
        @pl.when(valid(c))
        def _():
            for cp in tile_copies(h, c, slot):
                cp.start()

    def dloc_copies(c, slot):
        return [
            pltpu.make_async_copy(
                dydt.at[:, pl.ds(pl.multiple_of(q * eighth + c * Sd, Sd), Sd)],
                dloc.at[slot, s], dloc_sem.at[slot, s])
            for s, q in enumerate((i,) + plane_peers)
        ]

    def act_rows(q, c):
        return pl.ds(pl.multiple_of(q * eighth + c * Sd, Sd), Sd)

    def st_remote(c, slot):
        return [
            rcopy(
                st.at[slot, s], oact.at[act_rows(q, c), :],
                st_s.at[slot, s], oact_r.at[0], base + partner)
            for s, q in enumerate((i,) + plane_peers)
        ]

    wp_copy = rcopy(wall.at[0], wall.at[1], wp_s.at[0], wp_r.at[0], base + partner)

    def scalar_copy(ref, t, d):
        return rcopy(ref.at[me], ref.at[me], small_s.at[t], small_r.at[t], (me + d) % ndev)

    def row_copy(d):
        return rcopy(sa.at[i], sa.at[i], small_s.at[0], small_r.at[0], base + (i + d) % NR)

    def col_copy(d):
        return rcopy(sb.at[z], sb.at[z], small_s.at[1], small_r.at[1], ((z + d) % NZ) * NR + i)

    def lanes_of(v, width):
        n = v.shape[0]
        r_id = lax.broadcasted_iota(jnp.int32, (n, width), 0)
        l_id = lax.broadcasted_iota(jnp.int32, (n, width), 1)
        return jnp.sum(jnp.where(r_id == l_id, v, 0.0), axis=0, keepdims=True)

    def column_of(v, n):
        width = v.shape[1]
        r_id = lax.broadcasted_iota(jnp.int32, (n, width), 0)
        l_id = lax.broadcasted_iota(jnp.int32, (n, width), 1)
        return jnp.sum(jnp.where(r_id == l_id, v, 0.0), axis=1, keepdims=True)

    def total(v):
        return jnp.sum(jnp.sum(v, axis=1, keepdims=True), axis=0, keepdims=True)

    def pack_lanes(vals):
        lane = lax.broadcasted_iota(jnp.int32, (1, 128), 1)
        out = jnp.zeros((1, 128), F32)
        for t, v in enumerate(vals):
            out = jnp.where(lane == t, v, out)
        return out

    def lane_value(v, t):
        lane = lax.broadcasted_iota(jnp.int32, (1, 128), 1)
        return jnp.sum(jnp.where(lane == t, v, 0.0), axis=1, keepdims=True)

    m_gu = NR * gg.shape[0]
    n_gu = NZ * gg.shape[1]
    m_dn = NR * gdt.shape[1]
    n_dn = NZ * gdt.shape[0]
    mg = gg.shape[0]
    ng = gg.shape[1]
    md = gdt.shape[1]
    nd = gdt.shape[0]
    beta = hp[0]
    rho = hp[1]
    dcut = hp[2]

    def first_sums():
        tot = []
        for t, ref in enumerate((gg, gu)):
            g = ref[...]
            q = g * g + EPS_ONE
            rows = jnp.sum(q, axis=1, keepdims=True)
            sa[i, t] = jnp.sum(q, axis=0, keepdims=True)
            sb[z, t, :, pl.ds(0, 128)] = lanes_of(rows, 128)
            tot.append(total(rows))
        g = gdt[...]
        q = g * g + EPS_ONE
        n_sum = jnp.sum(q, axis=1, keepdims=True)
        sa[i, 2, :, pl.ds(0, 256)] = lanes_of(n_sum, 256)
        sb[z, 2] = jnp.sum(q, axis=0, keepdims=True)
        tot.append(total(n_sum))
        for ref in (wgf, wuf, wdf):
            w = ref[...]
            tot.append(total(w * w))
        for ref in (rg, ru, rd):
            tot.append(total(ref[...]))
        s1[me] = pack_lanes(tot)
        for d in range(1, NR):
            row_copy(d).start()
        for d in range(1, NZ):
            col_copy(d).start()

        def send(d, carry):
            scalar_copy(s1, 2, d).start()
            return carry

        lax.fori_loop(1, ndev, send, 0)

    def second_sums():
        some = sa.at[pl.ds(0, NR - 1)]
        rcopy(some, some, small_s.at[0], small_r.at[0], base + partner).wait_recv()
        some = sb.at[pl.ds(0, NZ - 1)]
        rcopy(some, some, small_s.at[1], small_r.at[1], base + partner).wait_recv()
        some = s1.at[pl.ds(0, ndev - 1)]
        rcopy(some, some, small_s.at[2], small_r.at[2], base + partner).wait_recv()
        tot = jnp.sum(s1[...], axis=0)
        asum = jnp.sum(sa[...], axis=0)
        bsum = jnp.sum(sb[...], axis=0)
        u_sq = []
        for t, (gref, rref, cref) in enumerate(((gg, rg, cg), (gu, ru, cu))):
            r_new = beta * rref[...] + (1.0 - beta) * (bsum[t][:, :mg] / n_gu)
            c_new = beta * cref[...] + (1.0 - beta) * (asum[t] / m_gu)
            q_mean = lane_value(tot, t) / (m_gu * n_gu)
            r_mean = beta * (lane_value(tot, 6 + t) / (NZ * m_gu)) + (1.0 - beta) * q_mean
            sv[pl.ds(2 * t, 1), pl.ds(0, mg)] = r_new
            sv[pl.ds(2 * t + 1, 1), :] = c_new
            u = gref[...] * lax.rsqrt(column_of(r_new, mg) * c_new / r_mean)
            gref[...] = u
            u_sq.append(total(u * u))
        r_new = beta * rd[...] + (1.0 - beta) * (bsum[2] / n_dn)
        c_new = beta * cd[...] + (1.0 - beta) * (asum[2][:, :nd] / m_dn)
        q_mean = lane_value(tot, 2) / (m_dn * n_dn)
        r_mean = beta * (lane_value(tot, 8) / (NZ * m_dn)) + (1.0 - beta) * q_mean
        sv[pl.ds(4, 1), pl.ds(0, md)] = r_new
        sv[pl.ds(5, 1), pl.ds(0, nd)] = c_new
        u = gdt[...] * lax.rsqrt(r_new * column_of(c_new, nd) / r_mean)
        gdt[...] = u
        u_sq.append(total(u * u))
        s2[me] = pack_lanes(u_sq)

        def send(d, carry):
            scalar_copy(s2, 3, d).start()
            return carry

        lax.fori_loop(1, ndev, send, 0)
        size = m_gu * n_gu
        sv[pl.ds(6, 1), pl.ds(0, 128)] = pack_lanes(
            [rho * jnp.maximum(EPS_TWO, jnp.sqrt(lane_value(tot, 3 + t) / size)) for t in range(3)])

    def third_sums():
        some = s2.at[pl.ds(0, ndev - 1)]
        rcopy(some, some, small_s.at[3], small_r.at[3], base + partner).wait_recv()
        rms_u = jnp.sqrt(jnp.sum(s2[...], axis=0) / (m_gu * n_gu))
        sv[pl.ds(7, 1), pl.ds(0, 128)] = sv[pl.ds(6, 1), pl.ds(0, 128)] / jnp.maximum(1.0, rms_u / dcut)

    for t, h in ((0, 3), (1, 0)):
        start_tile(h, 0, t)
    gg[...] = jnp.zeros_like(gg)
    gu[...] = jnp.zeros_like(gu)
    gdt[...] = jnp.zeros_like(gdt)
    sa[...] = jnp.zeros_like(sa)
    sb[...] = jnp.zeros_like(sb)
    sv[...] = jnp.zeros_like(sv)
    wg[...] = wgf[...].astype(BF16)
    wu[...] = wuf[...].astype(BF16)
    wdt[...] = wdf[...].astype(BF16)
    wall[0, 0] = wdt[...]
    pl.semaphore_wait(barrier, ndev - 1)

    @pl.when(z < NZ - 1)
    def _():
        rcopy(wdt, wall.at[0, 3], wu_s.at[0], w_r.at[2], up_id).start()

    @pl.when(z > 0)
    def _():
        rcopy(wdt, wall.at[0, 1], wd_s.at[0], w_r.at[0], dn_id).start()

    def send_own(c):
        @pl.when(c < C)
        def _():
            src = dydt.at[:, pl.ds(pl.multiple_of(i * eighth + c * Sd, Sd), Sd)]

            @pl.when(z < NZ - 1)
            def _():
                rcopy(src, dz.at[c, 2], dzu_s.at[0], dz_r.at[2, c], up_id).start()

            @pl.when(z > 0)
            def _():
                rcopy(src, dz.at[c, 0], dzd_s.at[0], dz_r.at[0, c], dn_id).start()

    def run_ahead(c, carry):
        send_own(c)
        return carry

    lax.fori_loop(0, AHEAD, run_ahead, 0)

    def step(k, carry):
        send_own(k + AHEAD)

        for d in (1, 2, 3):
            c = k - d
            ok = valid(c)

            @pl.when(both(k == d, z >= d))
            def _():
                rcopy(wdt, wall.at[0, 4 - d], wu_s.at[0], w_r.at[3 - d], up_id).wait_recv()
                if d < 3:
                    @pl.when(z < NZ - 1)
                    def _():
                        rcopy(wall.at[0, 4 - d], wall.at[0, 3 - d], wu_s.at[d], w_r.at[2 - d], up_id).start()

            @pl.when(both(k == d, NZ - 1 - z >= d))
            def _():
                rcopy(wdt, wall.at[0, d], wd_s.at[0], w_r.at[d - 1], dn_id).wait_recv()
                if d < 3:
                    @pl.when(z > 0)
                    def _():
                        rcopy(wall.at[0, d], wall.at[0, d + 1], wd_s.at[d], w_r.at[d], dn_id).start()

            @pl.when(both(ok, z >= d))
            def _():
                rcopy(dz.at[c, 3 - d], dz.at[c, 3 - d], dzu_s.at[0], dz_r.at[3 - d, c], up_id).wait_recv()
                if d < 3:
                    @pl.when(z < NZ - 1)
                    def _():
                        rcopy(dz.at[c, 3 - d], dz.at[c, 2 - d], dzu_s.at[d], dz_r.at[2 - d, c], up_id).start()

            @pl.when(both(ok, NZ - 1 - z >= d))
            def _():
                rcopy(dz.at[c, d - 1], dz.at[c, d - 1], dzd_s.at[0], dz_r.at[d - 1, c], dn_id).wait_recv()
                if d < 3:
                    @pl.when(z > 0)
                    def _():
                        rcopy(dz.at[c, d - 1], dz.at[c, d], dzd_s.at[d], dz_r.at[d, c], dn_id).start()

        cx = k - 3

        @pl.when(valid(cx))
        def _():
            for s, q in enumerate(plane_peers):
                rcopy(dz.at[cx], dxy.at[s, cx % SLOTS], dxy_s.at[s], dxy_r.at[s, cx], base + q).start()

        for h in range(NZ):
            dist = jnp.abs(z - h)
            c = k - HOME_LAG[h] - SKEW[h] - dist

            @pl.when(both(valid(c), z != h))
            def _():
                up_block(h, c).wait_recv()

                if h < NZ - 2:
                    @pl.when(both(z > h, z < NZ - 1))
                    def _():
                        up_block(h, c).start()

                if h > 1:
                    @pl.when(both(z < h, z > 0))
                    def _():
                        dn_block(h, c).start()


        @pl.when(k == C + 2)
        def _():
            first_sums()

        @pl.when(k == C + 4)
        def _():
            second_sums()

        order = (3, 0, 2, 1)
        for t, h in enumerate(order):
            slot = t % 2
            kt = k - SKEW[h]

            @pl.when(valid(kt))
            def _():
                for cp in tile_copies(h, kt, slot):
                    cp.wait()
                g = tg[slot]
                u = tu[slot]
                part[kt % 4, h] = mm_nt(wg[...], g) + mm_nt(wu[...], u)
                gg[...] += mm(txt[slot], g)
                gu[...] += mm(txt[slot], u)
                gdt[...] += mm(td[slot], txa[slot])

            hn = order[(t + 2) % 4]
            start_tile(hn, k + (t + 2) // 4 - SKEW[hn], slot)

            if h > 0:
                c = kt - z

                @pl.when(both(h > z, valid(c)))
                def _():
                    @pl.when(z > 0)
                    def _():
                        up_sum(h, c).wait_recv()
                        rsu[h - 1, c] = rsu[h - 1, c] + part[c % 4, h]

                    @pl.when(z == 0)
                    def _():
                        rsu[h - 1, c] = part[c % 4, h]

                    up_sum(h, c).start()

            if h < NZ - 1:
                c2 = kt - (NZ - 1 - z)

                @pl.when(both(h < z, valid(c2)))
                def _():
                    @pl.when(z < NZ - 1)
                    def _():
                        dn_sum(h, c2).wait_recv()
                        rsd[h, c2] = rsd[h, c2] + part[c2 % 4, h]

                    @pl.when(z == NZ - 1)
                    def _():
                        rsd[h, c2] = part[c2 % 4, h]

                    dn_sum(h, c2).start()

            c3 = kt - HOME_LAG[h]

            @pl.when(both(h == z, valid(c3)))
            def _():
                acc = part[c3 % 4, h]
                if h > 0:
                    up_sum(h, c3).wait_recv()
                    acc = acc + rsu[h - 1, c3]
                if h < NZ - 1:
                    dn_sum(h, c3).wait_recv()
                    acc = acc + rsd[h, c3]
                ag[h, c3] = acc.astype(BF16)
                if h < NZ - 1:
                    up_block(h, c3).start()
                if h > 0:
                    dn_block(h, c3).start()

        @pl.when(k == 3)
        def _():
            wp_copy.start()

        @pl.when(k == 5)
        def _():
            wp_copy.wait()

        cf = k - 4

        @pl.when(valid(cf))
        def _():
            for cp in dloc_copies(cf, cf % 2):
                cp.start()

        ca = k - 5
        slot_a = ca % 2

        @pl.when(valid(ca))
        def _():
            @pl.when(ca >= 2)
            def _():
                for cp in st_remote(ca - 2, slot_a):
                    cp.wait_send()

            locs = dloc_copies(ca, slot_a)
            outr = st_remote(ca, slot_a)
            for s, q in enumerate((i,) + plane_peers):
                locs[s].wait()
                if s == 0:
                    far = dz[ca]
                else:
                    rcopy(dz.at[ca], dxy.at[s - 1, ca % SLOTS], dxy_s.at[s - 1], dxy_r.at[s - 1, ca], base + xn).wait_recv()
                    far = dxy[s - 1, ca % SLOTS]
                lhs = jnp.concatenate([dloc[slot_a, s], far.reshape(3 * far.shape[1], Sd)], axis=0)
                w = wall[1].reshape(lhs.shape[0], wall.shape[3])
                st[slot_a, s] = mm_tn(lhs, w).astype(BF16)
                outr[s].start()
                w = wall[0].reshape(lhs.shape[0], wall.shape[3])
                oact[act_rows(q, ca), :] = mm_tn(lhs, w).astype(BF16)

        return carry

    lax.fori_loop(0, C + DRAIN, step, 0)
    third_sums()

    for c in (C - 2, C - 1):
        for cp in st_remote(c, c % 2):
            cp.wait_send()
    half = oact.at[pl.ds(0, T // 2), :]
    rcopy(half, half, st_s.at[0, 0], oact_r.at[0], base + partner).wait_recv()
    for h in (1, 2, 3):
        @pl.when(h > z)
        def _():
            rcopy(rsu.at[h - 1], rsu.at[h - 1], rsu_s.at[h - 1], rsu_r.at[h - 1, 0], up_id).wait_send()
    for h in (0, 1, 2):
        @pl.when(h < z)
        def _():
            rcopy(rsd.at[h], rsd.at[h], rsd_s.at[h], rsd_r.at[h, 0], dn_id).wait_send()
    for h in range(NZ):
        if h < NZ - 1:
            @pl.when(both(z >= h, z < NZ - 1))
            def _():
                rcopy(ag.at[h], ag.at[h], agu_s.at[h], ag_r.at[h, 0], up_id).wait_send()
        if h > 0:
            @pl.when(both(z <= h, z > 0))
            def _():
                rcopy(ag.at[h], ag.at[h], agd_s.at[h], ag_r.at[h, 0], dn_id).wait_send()
    for d in range(3):
        @pl.when(both(z >= d, z < NZ - 1))
        def _():
            rcopy(wdt, wdt, wu_s.at[d], w_r.at[0], up_id).wait_send()

        @pl.when(both(NZ - 1 - z >= d, z > 0))
        def _():
            rcopy(wdt, wdt, wd_s.at[d], w_r.at[0], dn_id).wait_send()
    for t, (ref, cnt) in enumerate(((sa, NR - 1), (sb, NZ - 1), (s1, ndev - 1), (s2, ndev - 1))):
        some = ref.at[pl.ds(0, cnt)]
        rcopy(some, some, small_s.at[t], small_r.at[t], base + partner).wait_send()
    dzall = dz.at[:, 0]
    for d in range(3):
        @pl.when(both(z >= d, z < NZ - 1))
        def _():
            rcopy(dzall, dzall, dzu_s.at[d], dz_r.at[0, 0], up_id).wait_send()

        @pl.when(both(NZ - 1 - z >= d, z > 0))
        def _():
            rcopy(dzall, dzall, dzd_s.at[d], dz_r.at[0, 0], dn_id).wait_send()
    for s in range(3):
        rcopy(dz, dz, dxy_s.at[s], dxy_r.at[s, 0], base + xn).wait_send()


def main_call(xt, xa, dyg, dyu, dydt, wg, wu, wdt, vecs, hp):
    T, ka = xa.shape
    m = xt.shape[0]
    n = dyg.shape[1]
    nd = dydt.shape[0]
    C = CHUNKS
    S = T // NZ // C
    Sd = T // NR // C
    dma = pltpu.SemaphoreType.DMA
    anyspec = pl.BlockSpec(memory_space=pl.ANY)
    vspec = pl.BlockSpec(memory_space=pltpu.VMEM)
    sspec = pl.BlockSpec(memory_space=pltpu.SMEM)
    scratch = [
        pltpu.VMEM((3, C, m, S), F32),
        pltpu.VMEM((3, C, m, S), F32),
        pltpu.VMEM((C, 3, nd, Sd), BF16),
        pltpu.VMEM((3, SLOTS, 3, nd, Sd), BF16),
        pltpu.VMEM((2, NZ, nd, ka), BF16),
        pltpu.VMEM((4, NZ, m, S), F32),
        pltpu.VMEM((2, m, S), BF16),
        pltpu.VMEM((2, S, ka), BF16),
        pltpu.VMEM((2, S, n), BF16),
        pltpu.VMEM((2, S, n), BF16),
        pltpu.VMEM((2, nd, S), BF16),
        pltpu.VMEM((2, 4, nd, Sd), BF16),
        pltpu.VMEM((2, 4, Sd, ka), BF16),
        pltpu.VMEM((m, n), BF16),
        pltpu.VMEM((m, n), BF16),
        pltpu.VMEM((nd, ka), BF16),
        pltpu.VMEM((NR, 3, 1, n), F32),
        pltpu.VMEM((NZ, 3, 1, 256), F32),
        pltpu.VMEM((NZ * NR, 1, 128), F32),
        pltpu.VMEM((NZ * NR, 1, 128), F32),
        dma((2, 5)), dma((2, 4)),
        dma((3, C)), dma((3, C)), dma((NZ, C)), dma((3, C)), dma((3, C)), dma((3,)), dma((1,)),
        dma((3,)), dma((3,)), dma((NZ,)), dma((NZ,)), dma((3,)), dma((3,)), dma((3,)), dma((3,)), dma((3,)), dma((1,)),
        dma((2, 4)), dma((1,)), dma((4,)), dma((4,)),
    ]
    return pl.pallas_call(
        kernel,
        out_shape=(
            pltpu.VMEM((NZ, C, m, S), BF16),
            pltpu.VMEM((T, ka), BF16),
            pltpu.VMEM((m, n), F32),
            pltpu.VMEM((m, n), F32),
            pltpu.VMEM((nd, ka), F32),
            pltpu.VMEM((8, n), F32),
        ),
        in_specs=[anyspec] * 5 + [vspec] * 9 + [sspec],
        out_specs=(vspec,) * 6,
        scratch_shapes=scratch,
        compiler_params=pltpu.CompilerParams(
            collective_id=0, has_side_effects=True, vmem_limit_bytes=40_000_000),
    )(xt, xa, dyg, dyu, dydt, wg, wu, wdt, *vecs, hp)


def final_kernel(
    ag, oact, ug, uu, ud, sv, wg, wu, wd,
    outt_o, oact_o, wg_o, wu_o, wd_o, rg_o, cg_o, ru_o, cu_o, rd_o, cd_o,
    sem,
):
    homes, C, _, S = ag.shape
    pltpu.make_async_copy(oact, oact_o, sem.at[0]).start()

    def send(c, carry):
        for h in range(homes):
            cols = pl.ds(pl.multiple_of(h * C * S + c * S, S), S)
            pltpu.make_async_copy(ag.at[h, c], outt_o.at[:, cols], sem.at[1]).start()
        return carry

    lax.fori_loop(0, C, send, 0)
    for t, (u, w, o) in enumerate(((ug, wg, wg_o), (uu, wu, wu_o), (ud, wd, wd_o))):
        o[...] = w[...] - sv[7:8, t:t + 1] * u[...]
    for t, o in enumerate((rg_o, cg_o, ru_o, cu_o, rd_o, cd_o)):
        o[...] = sv[t:t + 1, :o.shape[1]]
    pltpu.make_async_copy(oact, oact_o, sem.at[0]).wait()
    pltpu.make_async_copy(outt_o, outt_o, sem.at[1]).wait()


def final_call(ag, oact, ug, uu, ud, sv, wg, wu, wd):
    homes, C, m, S = ag.shape
    T, ka = oact.shape
    n = ug.shape[1]
    nd = ud.shape[0]
    anyspec = pl.BlockSpec(memory_space=pl.ANY)
    vspec = pl.BlockSpec(memory_space=pltpu.VMEM)
    shape = jax.ShapeDtypeStruct
    return pl.pallas_call(
        final_kernel,
        out_shape=(
            shape((m, T), BF16), shape((T, ka), BF16),
            shape((m, n), F32), shape((m, n), F32), shape((nd, ka), F32),
            shape((1, m), F32), shape((1, n), F32), shape((1, m), F32), shape((1, n), F32),
            shape((1, ka), F32), shape((1, nd), F32)),
        in_specs=[vspec] * 9,
        out_specs=(anyspec,) * 2 + (vspec,) * 9,
        scratch_shapes=[pltpu.SemaphoreType.DMA((2,))],
        compiler_params=pltpu.CompilerParams(vmem_limit_bytes=8_000_000),
    )(ag, oact, ug, uu, ud, sv, wg, wu, wd)


def solution(mesh):
    weight_spec = P('row', 'col')
    act_spec = P(None, 'row')
    grad_spec = P(None, 'col')
    in_specs = (weight_spec,) * 3 + (act_spec, act_spec) + (grad_spec,) * 3 + (P('row'), P('col')) * 3 + (P(),)
    out_specs = (weight_spec,) * 3 + (P('row'), P('col')) * 3 + (act_spec, act_spec)

    def body(w_gate, w_up, w_down, x_norm, x_act, dy_gate, dy_up, dy_down, r_gate, c_gate, r_up, c_up, r_down, c_down, hyper_params):
        wdt = w_down.T
        vecs = [v.reshape(1, -1) for v in (r_gate, c_gate, r_up, c_up, r_down, c_down)]
        held = main_call(
            x_norm.T, x_act, dy_gate, dy_up, dy_down.T, w_gate, w_up, wdt, vecs, hyper_params)
        held = [pltpu.with_memory_space_constraint(v, pltpu.VMEM) for v in held]
        outt, dx_act, new_gate, new_up, new_down_t, *stats = final_call(*held, w_gate, w_up, wdt)
        stats = [v.reshape(-1) for v in stats]
        return (new_gate, new_up, new_down_t.T, *stats, outt.T, dx_act)

    return jax.shard_map(body, mesh=mesh, in_specs=in_specs, out_specs=out_specs, check_vma=False)
```

```python
import jax
import jax.numpy as jnp
from jax import lax
from jax.experimental import pallas as pl
from jax.experimental.pallas import tpu as pltpu
from jax.sharding import PartitionSpec as P

EPS_ONE = 1e-30
EPS_TWO = 1e-3
CHUNKS = 32
NZ = 4
NR = 8
HOME_LAG = (3, 2, 2, 3)
SKEW = (0, 2, 2, 0)
UP_AFTER = ((3,), (), (2,), (1,))
DN_AFTER = ((), (0,), (), (1, 2))
HOME_AFTER = ((3,), (0,), (2,), (1,))
AHEAD = 3
SLOTS = 8
DRAIN = 6
F32 = jnp.float32
BF16 = jnp.bfloat16


def mm(a, b):
    return lax.dot_general(a, b, (((1,), (0,)), ((), ())), preferred_element_type=F32)


def mm_nt(a, b):
    return lax.dot_general(a, b, (((1,), (1,)), ((), ())), preferred_element_type=F32)


def mm_tn(a, b):
    return lax.dot_general(a, b, (((0,), (0,)), ((), ())), preferred_element_type=F32)


def kernel(
    xt, xa, dyg, dyu, dydt, wgh, wuh, wdh, rg, cg, ru, cu, rd, cd, hp,
    ag, oact, gg, gu, gdt, sv,
    rsu, rsd, dz, dxy, wall, part, txt, txa, tg, tu, td, dloc, st,
    wg, wu, wdt, sa, sb, s1, s2, wgf, wuf, wdf,
    tile_sem, dloc_sem, rsu_r, rsd_r, ag_r, dz_r, dxy_r, w_r, wp_r,
    rsu_s, rsd_s, agu_s, agd_s, dzu_s, dzd_s, dxy_s, wu_s, wd_s, wp_s,
    st_s, oact_r, small_s, small_r, win_sem,
):
    z = lax.axis_index("col")
    i = lax.axis_index("row")
    core = i % 2
    xx = (i // 2) % 2
    yy = i // 4
    base = z * NR
    partner = i + 1 - 2 * core
    xn = i + 2 * (1 - 2 * xx)
    yn = i + 4 * (1 - 2 * yy)
    dg = xn + 4 * (1 - 2 * yy)
    plane_peers = (xn, yn, dg)
    C = rsu.shape[1]
    S = rsu.shape[3]
    Sd = dz.shape[3]
    T = xa.shape[0]
    home_len = T // NZ
    eighth = T // NR
    up_id = base + NR + i
    dn_id = base - NR + i

    def rcopy(src, dst, ssem, rsem, dev):
        return pltpu.make_async_remote_copy(
            src, dst, ssem, rsem, device_id=dev, device_id_type=pl.DeviceIdType.LOGICAL
        )

    def up_sum(h, c):
        return rcopy(rsu.at[h - 1, c], rsu.at[h - 1, c], rsu_s.at[h - 1], rsu_r.at[h - 1, c], up_id)

    def dn_sum(h, c):
        return rcopy(rsd.at[h, c], rsd.at[h, c], rsd_s.at[h], rsd_r.at[h, c], dn_id)

    def up_block(h, c):
        return rcopy(ag.at[h, c], ag.at[h, c], agu_s.at[h], ag_r.at[h, c], up_id)

    def dn_block(h, c):
        return rcopy(ag.at[h, c], ag.at[h, c], agd_s.at[h], ag_r.at[h, c], dn_id)

    def both(a, b):
        return jnp.logical_and(a, b)

    def valid(c):
        return both(c >= 0, c < C)

    barrier = pltpu.get_barrier_semaphore()
    me = base + i
    ndev = NZ * NR

    near = [base + q for q in (*plane_peers, partner)] + [((z + d) % NZ) * NR + i for d in (1, NZ - 1)]
    for dev in near:
        pl.semaphore_signal(barrier, inc=1, device_id=dev, device_id_type=pl.DeviceIdType.LOGICAL)

    def tile_copies(h, c, slot):
        t0 = pl.multiple_of(h * home_len + c * S, S)
        rows = pl.ds(t0, S)
        return [
            pltpu.make_async_copy(xt.at[:, rows], txt.at[slot], tile_sem.at[slot, 0]),
            pltpu.make_async_copy(xa.at[rows, :], txa.at[slot], tile_sem.at[slot, 1]),
            pltpu.make_async_copy(dyg.at[rows, :], tg.at[slot], tile_sem.at[slot, 2]),
            pltpu.make_async_copy(dyu.at[rows, :], tu.at[slot], tile_sem.at[slot, 3]),
            pltpu.make_async_copy(dydt.at[:, rows], td.at[slot], tile_sem.at[slot, 4]),
        ]

    def start_tile(h, c, slot):
        @pl.when(valid(c))
        def _():
            for cp in tile_copies(h, c, slot):
                cp.start()

    def dloc_copies(c, slot):
        return [
            pltpu.make_async_copy(
                dydt.at[:, pl.ds(pl.multiple_of(q * eighth + c * Sd, Sd), Sd)],
                dloc.at[slot, s], dloc_sem.at[slot, s])
            for s, q in enumerate((i,) + plane_peers)
        ]

    def act_rows(q, c):
        return pl.ds(pl.multiple_of(q * eighth + c * Sd, Sd), Sd)

    def st_remote(c, slot):
        return [
            rcopy(
                st.at[slot, s], oact.at[act_rows(q, c), :],
                st_s.at[slot, s], oact_r.at[0], base + partner)
            for s, q in enumerate((i,) + plane_peers)
        ]

    wp_copy = rcopy(wall.at[0], wall.at[1], wp_s.at[0], wp_r.at[0], base + partner)

    def scalar_copy(ref, t, d):
        return rcopy(ref.at[me], ref.at[me], small_s.at[t], small_r.at[t], (me + d) % ndev)

    def row_copy(d):
        return rcopy(sa.at[i], sa.at[i], small_s.at[0], small_r.at[0], base + (i + d) % NR)

    def col_copy(d):
        return rcopy(sb.at[z], sb.at[z], small_s.at[1], small_r.at[1], ((z + d) % NZ) * NR + i)

    def lanes_of(v, width):
        n = v.shape[0]
        r_id = lax.broadcasted_iota(jnp.int32, (n, width), 0)
        l_id = lax.broadcasted_iota(jnp.int32, (n, width), 1)
        return jnp.sum(jnp.where(r_id == l_id, v, 0.0), axis=0, keepdims=True)

    def column_of(v, n):
        width = v.shape[1]
        r_id = lax.broadcasted_iota(jnp.int32, (n, width), 0)
        l_id = lax.broadcasted_iota(jnp.int32, (n, width), 1)
        return jnp.sum(jnp.where(r_id == l_id, v, 0.0), axis=1, keepdims=True)

    def total(v):
        return jnp.sum(jnp.sum(v, axis=1, keepdims=True), axis=0, keepdims=True)

    def pack_lanes(vals):
        lane = lax.broadcasted_iota(jnp.int32, (1, 128), 1)
        out = jnp.zeros((1, 128), F32)
        for t, v in enumerate(vals):
            out = jnp.where(lane == t, v, out)
        return out

    def lane_value(v, t):
        lane = lax.broadcasted_iota(jnp.int32, (1, 128), 1)
        return jnp.sum(jnp.where(lane == t, v, 0.0), axis=1, keepdims=True)

    m_gu = NR * gg.shape[0]
    n_gu = NZ * gg.shape[1]
    m_dn = NR * gdt.shape[1]
    n_dn = NZ * gdt.shape[0]
    mg = gg.shape[0]
    ng = gg.shape[1]
    md = gdt.shape[1]
    nd = gdt.shape[0]
    beta = hp[0]
    rho = hp[1]
    dcut = hp[2]

    def first_sums():
        tot = []
        for t, ref in enumerate((gg, gu)):
            g = ref[...]
            q = g * g + EPS_ONE
            rows = jnp.sum(q, axis=1, keepdims=True)
            sa[i, t] = jnp.sum(q, axis=0, keepdims=True)
            sb[z, t, :, pl.ds(0, 128)] = lanes_of(rows, 128)
            tot.append(total(rows))
        g = gdt[...]
        q = g * g + EPS_ONE
        n_sum = jnp.sum(q, axis=1, keepdims=True)
        sa[i, 2, :, pl.ds(0, 256)] = lanes_of(n_sum, 256)
        sb[z, 2] = jnp.sum(q, axis=0, keepdims=True)
        tot.append(total(n_sum))
        for ref in (wgf, wuf, wdf):
            w = ref[...]
            tot.append(total(w * w))
        for ref in (rg, ru, rd):
            tot.append(total(ref[...]))
        s1[me] = pack_lanes(tot)
        for d in range(1, NR):
            row_copy(d).start()
        for d in range(1, NZ):
            col_copy(d).start()

        def send(d, carry):
            scalar_copy(s1, 2, d).start()
            return carry

        lax.fori_loop(1, ndev, send, 0)

    def second_sums():
        some = sa.at[pl.ds(0, NR - 1)]
        rcopy(some, some, small_s.at[0], small_r.at[0], base + partner).wait_recv()
        some = sb.at[pl.ds(0, NZ - 1)]
        rcopy(some, some, small_s.at[1], small_r.at[1], base + partner).wait_recv()
        some = s1.at[pl.ds(0, ndev - 1)]
        rcopy(some, some, small_s.at[2], small_r.at[2], base + partner).wait_recv()
        tot = jnp.sum(s1[...], axis=0)
        asum = jnp.sum(sa[...], axis=0)
        bsum = jnp.sum(sb[...], axis=0)
        u_sq = []
        for t, (gref, rref, cref) in enumerate(((gg, rg, cg), (gu, ru, cu))):
            r_new = beta * rref[...] + (1.0 - beta) * (bsum[t][:, :mg] / n_gu)
            c_new = beta * cref[...] + (1.0 - beta) * (asum[t] / m_gu)
            q_mean = lane_value(tot, t) / (m_gu * n_gu)
            r_mean = beta * (lane_value(tot, 6 + t) / (NZ * m_gu)) + (1.0 - beta) * q_mean
            sv[pl.ds(2 * t, 1), pl.ds(0, mg)] = r_new
            sv[pl.ds(2 * t + 1, 1), :] = c_new
            u = gref[...] * lax.rsqrt(column_of(r_new, mg) * c_new / r_mean)
            gref[...] = u
            u_sq.append(total(u * u))
        r_new = beta * rd[...] + (1.0 - beta) * (bsum[2] / n_dn)
        c_new = beta * cd[...] + (1.0 - beta) * (asum[2][:, :nd] / m_dn)
        q_mean = lane_value(tot, 2) / (m_dn * n_dn)
        r_mean = beta * (lane_value(tot, 8) / (NZ * m_dn)) + (1.0 - beta) * q_mean
        sv[pl.ds(4, 1), pl.ds(0, md)] = r_new
        sv[pl.ds(5, 1), pl.ds(0, nd)] = c_new
        u = gdt[...] * lax.rsqrt(r_new * column_of(c_new, nd) / r_mean)
        gdt[...] = u
        u_sq.append(total(u * u))
        s2[me] = pack_lanes(u_sq)

        def send(d, carry):
            scalar_copy(s2, 3, d).start()
            return carry

        lax.fori_loop(1, ndev, send, 0)
        size = m_gu * n_gu
        sv[pl.ds(6, 1), pl.ds(0, 128)] = pack_lanes(
            [rho * jnp.maximum(EPS_TWO, jnp.sqrt(lane_value(tot, 3 + t) / size)) for t in range(3)])

    def third_sums():
        some = s2.at[pl.ds(0, ndev - 1)]
        rcopy(some, some, small_s.at[3], small_r.at[3], base + partner).wait_recv()
        rms_u = jnp.sqrt(jnp.sum(s2[...], axis=0) / (m_gu * n_gu))
        sv[pl.ds(7, 1), pl.ds(0, 128)] = sv[pl.ds(6, 1), pl.ds(0, 128)] / jnp.maximum(1.0, rms_u / dcut)

    w_in = [
        pltpu.make_async_copy(src, dst, win_sem.at[t])
        for t, (src, dst) in enumerate(((wgh, wgf), (wuh, wuf), (wdh, wdf)))
    ]
    for cp in w_in:
        cp.start()
    for t, h in ((0, 3), (1, 0)):
        start_tile(h, 0, t)
    gg[...] = jnp.zeros_like(gg)
    gu[...] = jnp.zeros_like(gu)
    gdt[...] = jnp.zeros_like(gdt)
    sa[...] = jnp.zeros_like(sa)
    sb[...] = jnp.zeros_like(sb)
    sv[...] = jnp.zeros_like(sv)
    for cp in w_in:
        cp.wait()
    wg[...] = wgf[...].astype(BF16)
    wu[...] = wuf[...].astype(BF16)
    wdt[...] = wdf[...].astype(BF16)
    wall[0, 0] = wdt[...]
    pl.semaphore_wait(barrier, len(near))

    @pl.when(z < NZ - 1)
    def _():
        rcopy(wdt, wall.at[0, 3], wu_s.at[0], w_r.at[2], up_id).start()

    @pl.when(z > 0)
    def _():
        rcopy(wdt, wall.at[0, 1], wd_s.at[0], w_r.at[0], dn_id).start()

    def send_own(c):
        @pl.when(c < C)
        def _():
            src = dydt.at[:, pl.ds(pl.multiple_of(i * eighth + c * Sd, Sd), Sd)]

            @pl.when(z < NZ - 1)
            def _():
                rcopy(src, dz.at[c, 2], dzu_s.at[0], dz_r.at[2, c], up_id).start()

            @pl.when(z > 0)
            def _():
                rcopy(src, dz.at[c, 0], dzd_s.at[0], dz_r.at[0, c], dn_id).start()

    def run_ahead(c, carry):
        send_own(c)
        return carry

    lax.fori_loop(0, AHEAD, run_ahead, 0)

    def step(k, carry):
        send_own(k + AHEAD)

        for d in (1, 2, 3):
            c = k - d
            ok = valid(c)

            @pl.when(both(k == d, z >= d))
            def _():
                rcopy(wdt, wall.at[0, 4 - d], wu_s.at[0], w_r.at[3 - d], up_id).wait_recv()
                if d < 3:
                    @pl.when(z < NZ - 1)
                    def _():
                        rcopy(wall.at[0, 4 - d], wall.at[0, 3 - d], wu_s.at[d], w_r.at[2 - d], up_id).start()

            @pl.when(both(k == d, NZ - 1 - z >= d))
            def _():
                rcopy(wdt, wall.at[0, d], wd_s.at[0], w_r.at[d - 1], dn_id).wait_recv()
                if d < 3:
                    @pl.when(z > 0)
                    def _():
                        rcopy(wall.at[0, d], wall.at[0, d + 1], wd_s.at[d], w_r.at[d], dn_id).start()

            @pl.when(both(ok, z >= d))
            def _():
                rcopy(dz.at[c, 3 - d], dz.at[c, 3 - d], dzu_s.at[0], dz_r.at[3 - d, c], up_id).wait_recv()
                if d < 3:
                    @pl.when(z < NZ - 1)
                    def _():
                        rcopy(dz.at[c, 3 - d], dz.at[c, 2 - d], dzu_s.at[d], dz_r.at[2 - d, c], up_id).start()

            @pl.when(both(ok, NZ - 1 - z >= d))
            def _():
                rcopy(dz.at[c, d - 1], dz.at[c, d - 1], dzd_s.at[0], dz_r.at[d - 1, c], dn_id).wait_recv()
                if d < 3:
                    @pl.when(z > 0)
                    def _():
                        rcopy(dz.at[c, d - 1], dz.at[c, d], dzd_s.at[d], dz_r.at[d, c], dn_id).start()

        cx = k - 3

        @pl.when(valid(cx))
        def _():
            for s, q in enumerate(plane_peers):
                rcopy(dz.at[cx], dxy.at[s, cx % SLOTS], dxy_s.at[s], dxy_r.at[s, cx], base + q).start()

        for h in range(NZ):
            dist = jnp.abs(z - h)
            c = k - HOME_LAG[h] - SKEW[h] - dist

            @pl.when(both(valid(c), z != h))
            def _():
                up_block(h, c).wait_recv()

                if h < NZ - 2:
                    @pl.when(both(z > h, z < NZ - 1))
                    def _():
                        up_block(h, c).start()

                if h > 1:
                    @pl.when(both(z < h, z > 0))
                    def _():
                        dn_block(h, c).start()


        def pass_up(h):
            if h > 0:
                c = k - SKEW[h] - z

                @pl.when(both(h > z, valid(c)))
                def _():
                    @pl.when(z > 0)
                    def _():
                        up_sum(h, c).wait_recv()
                        rsu[h - 1, c] = rsu[h - 1, c] + part[c % 4, h]

                    @pl.when(z == 0)
                    def _():
                        rsu[h - 1, c] = part[c % 4, h]

                    up_sum(h, c).start()

        def pass_dn(h):
            if h < NZ - 1:
                c2 = k - SKEW[h] - (NZ - 1 - z)

                @pl.when(both(h < z, valid(c2)))
                def _():
                    @pl.when(z < NZ - 1)
                    def _():
                        dn_sum(h, c2).wait_recv()
                        rsd[h, c2] = rsd[h, c2] + part[c2 % 4, h]

                    @pl.when(z == NZ - 1)
                    def _():
                        rsd[h, c2] = part[c2 % 4, h]

                    dn_sum(h, c2).start()

        def finish(h):
            c3 = k - SKEW[h] - HOME_LAG[h]

            @pl.when(both(h == z, valid(c3)))
            def _():
                acc = part[c3 % 4, h]
                if h > 0:
                    up_sum(h, c3).wait_recv()
                    acc = acc + rsu[h - 1, c3]
                if h < NZ - 1:
                    dn_sum(h, c3).wait_recv()
                    acc = acc + rsd[h, c3]
                ag[h, c3] = acc.astype(BF16)
                if h < NZ - 1:
                    up_block(h, c3).start()
                if h > 0:
                    dn_block(h, c3).start()

        order = (3, 0, 2, 1)
        for t, h in enumerate(order):
            slot = t % 2
            kt = k - SKEW[h]

            @pl.when(valid(kt))
            def _():
                for cp in tile_copies(h, kt, slot):
                    cp.wait()
                g = tg[slot]
                u = tu[slot]
                part[kt % 4, h] = mm_nt(wg[...], g) + mm_nt(wu[...], u)
                gg[...] += mm(txt[slot], g)
                gu[...] += mm(txt[slot], u)
                gdt[...] += mm(td[slot], txa[slot])

            hn = order[(t + 2) % 4]
            start_tile(hn, k + (t + 2) // 4 - SKEW[hn], slot)

            for hu in UP_AFTER[t]:
                pass_up(hu)
            for hd in DN_AFTER[t]:
                pass_dn(hd)
            for hh in HOME_AFTER[t]:
                finish(hh)

        @pl.when(k == C + 2)
        def _():
            first_sums()

        @pl.when(k == C + 4)
        def _():
            second_sums()

        @pl.when(k == 3)
        def _():
            wp_copy.start()

        @pl.when(k == 5)
        def _():
            wp_copy.wait()

        cf = k - 4

        @pl.when(valid(cf))
        def _():
            for cp in dloc_copies(cf, cf % 2):
                cp.start()

        ca = k - 5
        slot_a = ca % 2

        @pl.when(valid(ca))
        def _():
            @pl.when(ca >= 2)
            def _():
                for cp in st_remote(ca - 2, slot_a):
                    cp.wait_send()

            locs = dloc_copies(ca, slot_a)
            outr = st_remote(ca, slot_a)
            for s, q in enumerate((i,) + plane_peers):
                locs[s].wait()
                if s == 0:
                    far = dz[ca]
                else:
                    rcopy(dz.at[ca], dxy.at[s - 1, ca % SLOTS], dxy_s.at[s - 1], dxy_r.at[s - 1, ca], base + xn).wait_recv()
                    far = dxy[s - 1, ca % SLOTS]
                lhs = jnp.concatenate([dloc[slot_a, s], far.reshape(3 * far.shape[1], Sd)], axis=0)
                w = wall[1].reshape(lhs.shape[0], wall.shape[3])
                st[slot_a, s] = mm_tn(lhs, w).astype(BF16)
                outr[s].start()
                w = wall[0].reshape(lhs.shape[0], wall.shape[3])
                oact[act_rows(q, ca), :] = mm_tn(lhs, w).astype(BF16)

        return carry

    lax.fori_loop(0, C + DRAIN, step, 0)
    third_sums()

    for c in (C - 2, C - 1):
        for cp in st_remote(c, c % 2):
            cp.wait_send()
    half = oact.at[pl.ds(0, T // 2), :]
    rcopy(half, half, st_s.at[0, 0], oact_r.at[0], base + partner).wait_recv()
    for h in (1, 2, 3):
        @pl.when(h > z)
        def _():
            rcopy(rsu.at[h - 1], rsu.at[h - 1], rsu_s.at[h - 1], rsu_r.at[h - 1, 0], up_id).wait_send()
    for h in (0, 1, 2):
        @pl.when(h < z)
        def _():
            rcopy(rsd.at[h], rsd.at[h], rsd_s.at[h], rsd_r.at[h, 0], dn_id).wait_send()
    for h in range(NZ):
        if h < NZ - 1:
            @pl.when(both(z >= h, z < NZ - 1))
            def _():
                rcopy(ag.at[h], ag.at[h], agu_s.at[h], ag_r.at[h, 0], up_id).wait_send()
        if h > 0:
            @pl.when(both(z <= h, z > 0))
            def _():
                rcopy(ag.at[h], ag.at[h], agd_s.at[h], ag_r.at[h, 0], dn_id).wait_send()
    for d in range(3):
        @pl.when(both(z >= d, z < NZ - 1))
        def _():
            rcopy(wdt, wdt, wu_s.at[d], w_r.at[0], up_id).wait_send()

        @pl.when(both(NZ - 1 - z >= d, z > 0))
        def _():
            rcopy(wdt, wdt, wd_s.at[d], w_r.at[0], dn_id).wait_send()
    for t, (ref, cnt) in enumerate(((sa, NR - 1), (sb, NZ - 1), (s1, ndev - 1), (s2, ndev - 1))):
        some = ref.at[pl.ds(0, cnt)]
        rcopy(some, some, small_s.at[t], small_r.at[t], base + partner).wait_send()
    dzall = dz.at[:, 0]
    for d in range(3):
        @pl.when(both(z >= d, z < NZ - 1))
        def _():
            rcopy(dzall, dzall, dzu_s.at[d], dz_r.at[0, 0], up_id).wait_send()

        @pl.when(both(NZ - 1 - z >= d, z > 0))
        def _():
            rcopy(dzall, dzall, dzd_s.at[d], dz_r.at[0, 0], dn_id).wait_send()
    for s in range(3):
        rcopy(dz, dz, dxy_s.at[s], dxy_r.at[s, 0], base + xn).wait_send()


def main_call(xt, xa, dyg, dyu, dydt, wg, wu, wdt, vecs, hp):
    T, ka = xa.shape
    m = xt.shape[0]
    n = dyg.shape[1]
    nd = dydt.shape[0]
    C = CHUNKS
    S = T // NZ // C
    Sd = T // NR // C
    dma = pltpu.SemaphoreType.DMA
    anyspec = pl.BlockSpec(memory_space=pl.ANY)
    vspec = pl.BlockSpec(memory_space=pltpu.VMEM)
    sspec = pl.BlockSpec(memory_space=pltpu.SMEM)
    scratch = [
        pltpu.VMEM((3, C, m, S), F32),
        pltpu.VMEM((3, C, m, S), F32),
        pltpu.VMEM((C, 3, nd, Sd), BF16),
        pltpu.VMEM((3, SLOTS, 3, nd, Sd), BF16),
        pltpu.VMEM((2, NZ, nd, ka), BF16),
        pltpu.VMEM((4, NZ, m, S), F32),
        pltpu.VMEM((2, m, S), BF16),
        pltpu.VMEM((2, S, ka), BF16),
        pltpu.VMEM((2, S, n), BF16),
        pltpu.VMEM((2, S, n), BF16),
        pltpu.VMEM((2, nd, S), BF16),
        pltpu.VMEM((2, 4, nd, Sd), BF16),
        pltpu.VMEM((2, 4, Sd, ka), BF16),
        pltpu.VMEM((m, n), BF16),
        pltpu.VMEM((m, n), BF16),
        pltpu.VMEM((nd, ka), BF16),
        pltpu.VMEM((NR, 3, 1, n), F32),
        pltpu.VMEM((NZ, 3, 1, 256), F32),
        pltpu.VMEM((NZ * NR, 1, 128), F32),
        pltpu.VMEM((NZ * NR, 1, 128), F32),
        pltpu.VMEM((m, n), F32),
        pltpu.VMEM((m, n), F32),
        pltpu.VMEM((nd, ka), F32),
        dma((2, 5)), dma((2, 4)),
        dma((3, C)), dma((3, C)), dma((NZ, C)), dma((3, C)), dma((3, C)), dma((3,)), dma((1,)),
        dma((3,)), dma((3,)), dma((NZ,)), dma((NZ,)), dma((3,)), dma((3,)), dma((3,)), dma((3,)), dma((3,)), dma((1,)),
        dma((2, 4)), dma((1,)), dma((4,)), dma((4,)), dma((3,)),
    ]
    return pl.pallas_call(
        kernel,
        out_shape=(
            pltpu.VMEM((NZ, C, m, S), BF16),
            pltpu.VMEM((T, ka), BF16),
            pltpu.VMEM((m, n), F32),
            pltpu.VMEM((m, n), F32),
            pltpu.VMEM((nd, ka), F32),
            pltpu.VMEM((8, n), F32),
        ),
        in_specs=[anyspec] * 8 + [vspec] * 6 + [sspec],
        out_specs=(vspec,) * 6,
        scratch_shapes=scratch,
        compiler_params=pltpu.CompilerParams(
            collective_id=0, has_side_effects=True, vmem_limit_bytes=40_000_000),
    )(xt, xa, dyg, dyu, dydt, wg, wu, wdt, *vecs, hp)


def final_kernel(
    ag, oact, ug, uu, ud, sv, wg, wu, wd,
    outt_o, oact_o, wg_o, wu_o, wd_o, rg_o, cg_o, ru_o, cu_o, rd_o, cd_o,
    sem,
):
    homes, C, _, S = ag.shape
    pltpu.make_async_copy(oact, oact_o, sem.at[0]).start()

    def send(c, carry):
        for h in range(homes):
            cols = pl.ds(pl.multiple_of(h * C * S + c * S, S), S)
            pltpu.make_async_copy(ag.at[h, c], outt_o.at[:, cols], sem.at[1]).start()
        return carry

    lax.fori_loop(0, C, send, 0)
    for t, (u, w, o) in enumerate(((ug, wg, wg_o), (uu, wu, wu_o), (ud, wd, wd_o))):
        o[...] = w[...] - sv[7:8, t:t + 1] * u[...]
    for t, o in enumerate((rg_o, cg_o, ru_o, cu_o, rd_o, cd_o)):
        o[...] = sv[t:t + 1, :o.shape[1]]
    pltpu.make_async_copy(oact, oact_o, sem.at[0]).wait()
    pltpu.make_async_copy(outt_o, outt_o, sem.at[1]).wait()


def final_call(ag, oact, ug, uu, ud, sv, wg, wu, wd):
    homes, C, m, S = ag.shape
    T, ka = oact.shape
    n = ug.shape[1]
    nd = ud.shape[0]
    anyspec = pl.BlockSpec(memory_space=pl.ANY)
    vspec = pl.BlockSpec(memory_space=pltpu.VMEM)
    shape = jax.ShapeDtypeStruct
    return pl.pallas_call(
        final_kernel,
        out_shape=(
            shape((m, T), BF16), shape((T, ka), BF16),
            shape((m, n), F32), shape((m, n), F32), shape((nd, ka), F32),
            shape((1, m), F32), shape((1, n), F32), shape((1, m), F32), shape((1, n), F32),
            shape((1, ka), F32), shape((1, nd), F32)),
        in_specs=[vspec] * 9,
        out_specs=(anyspec,) * 2 + (vspec,) * 9,
        scratch_shapes=[pltpu.SemaphoreType.DMA((2,))],
        compiler_params=pltpu.CompilerParams(vmem_limit_bytes=8_000_000),
    )(ag, oact, ug, uu, ud, sv, wg, wu, wd)


def solution(mesh):
    weight_spec = P('row', 'col')
    act_spec = P(None, 'row')
    grad_spec = P(None, 'col')
    in_specs = (weight_spec,) * 3 + (act_spec, act_spec) + (grad_spec,) * 3 + (P('row'), P('col')) * 3 + (P(),)
    out_specs = (weight_spec,) * 3 + (P('row'), P('col')) * 3 + (act_spec, act_spec)

    def body(w_gate, w_up, w_down, x_norm, x_act, dy_gate, dy_up, dy_down, r_gate, c_gate, r_up, c_up, r_down, c_down, hyper_params):
        wdt = w_down.T
        vecs = [v.reshape(1, -1) for v in (r_gate, c_gate, r_up, c_up, r_down, c_down)]
        held = main_call(
            x_norm.T, x_act, dy_gate, dy_up, dy_down.T, w_gate, w_up, wdt, vecs, hyper_params)
        held = [pltpu.with_memory_space_constraint(v, pltpu.VMEM) for v in held]
        outt, dx_act, new_gate, new_up, new_down_t, *stats = final_call(*held, w_gate, w_up, wdt)
        stats = [v.reshape(-1) for v in stats]
        return (new_gate, new_up, new_down_t.T, *stats, outt.T, dx_act)

    return jax.shard_map(body, mesh=mesh, in_specs=in_specs, out_specs=out_specs, check_vma=False)
```
